64 devices in a mesh: rep: 8 (over x, y, core), dp: 8 (over z).
Axes of the slice: x: 2, y: 2, z: 8, core: 2. Of those that a mesh axis runs over, the one named last changes fastest.
The devices are a block of a 4x4x8 slice.
Arguments:
- x: bfloat16 [64, 2048, 512], P(('rep', 'dp')), parts along dimension 0
- dy: bfloat16 [64, 2048, 512], P(('rep', 'dp')), parts along dimension 0
- w_gate: bfloat16 [2, 512, 2560], replicated
- w_up: bfloat16 [2, 512, 2560], replicated
- w_down: bfloat16 [2, 2560, 512], replicated
- m_w_gate: float32 [2, 512, 2560], replicated
- m_w_up: float32 [2, 512, 2560], replicated
- m_w_down: float32 [2, 2560, 512], replicated
- v_w_gate: float32 [2, 512, 2560], replicated
- v_w_up: float32 [2, 512, 2560], replicated
- v_w_down: float32 [2, 2560, 512], replicated
Outputs:
- output 1: bfloat16 [16, 512, 2560], P('rep'), parts along dimension 0
- output 2: bfloat16 [16, 512, 2560], P('rep'), parts along dimension 0
- output 3: bfloat16 [16, 2560, 512], P('rep'), parts along dimension 0
- output 4: float32 [16, 512, 2560], P('rep'), parts along dimension 0
- output 5: float32 [16, 512, 2560], P('rep'), parts along dimension 0
- output 6: float32 [16, 2560, 512], P('rep'), parts along dimension 0
- output 7: float32 [16, 512, 2560], P('rep'), parts along dimension 0
- output 8: float32 [16, 512, 2560], P('rep'), parts along dimension 0
- output 9: float32 [16, 2560, 512], P('rep'), parts along dimension 0
There are 8 independent parts. The reference program is written for one: setup_inputs(seed, part) draws one part's arguments, and reference() takes and returns one part's arrays. A program takes and returns all parts, laid end to end along the dimension named above; an argument that names none is the same for every part.
All inputs are finite; a program needn't handle non-finite values.
Results may differ from the reference program's by a relative error of at most 0.022.
Values are sent between devices in bfloat16 or wider.
A program may use at most 768 MiB of HBM per device.

```python
import jax
import jax.numpy as jnp
from jax import lax

SEQUENCES = 8
TOKENS = 2048
D = 512
FF = 2560
LAYERS = 2
NAMES = ("w_gate", "w_up", "w_down")
SHAPES = {"w_gate": (LAYERS, D, FF), "w_up": (LAYERS, D, FF), "w_down": (LAYERS, FF, D)}


def bump(key, n, height):
    away = (jnp.arange(n, dtype=jnp.int32) - jax.random.randint(key, (), 0, n, jnp.int32)) % n
    return jnp.where(away < n // 8, height, 1.0)


def together(key, own, strength):
    shared = jax.random.normal(key, own.shape[1:], jnp.float32)
    return (own + strength * shared) * lax.rsqrt(1 + strength * strength)


def setup_inputs(seed: int = 0, part: int = 0) -> dict:
    kx, kdy, ka, kb, kz, kf, kh, kl, *keys = jax.random.split(jax.random.key(seed), 8 + 3 * len(NAMES))
    kx, kdy, ka, kb = (jax.random.fold_in(k, part) for k in (kx, kdy, ka, kb))
    kw, km, kv = (keys[i::3] for i in range(3))
    shape = (SEQUENCES, TOKENS, D)
    much_x, much_dy = jax.random.uniform(kz, (2,), jnp.float32, 0.0, 1.0)
    loud = 2.0 ** jax.random.uniform(jax.random.fold_in(kz, 1), (), jnp.float32, -1.0, 2.0)
    layers = 2.0 ** jax.random.uniform(kl, (LAYERS, 1, 1), jnp.float32, -1.0, 1.0)
    x = together(ka, jax.random.normal(kx, shape, jnp.float32), much_x) * bump(kf, D, 4.0)
    dy = together(kb, jax.random.normal(kdy, shape, jnp.float32), much_dy)
    drawn = {"x": x.astype(jnp.bfloat16), "dy": (loud * dy * (SEQUENCES * TOKENS) ** -0.5).astype(jnp.bfloat16)}
    for key, name in zip(kw, NAMES, strict=True):
        w = jax.random.normal(key, SHAPES[name], jnp.float32) * SHAPES[name][1] ** -0.5
        drawn[name] = (w * {"w_gate": 1.0, "w_up": bump(kh, FF, 4.0), "w_down": layers}[name]).astype(jnp.bfloat16)
    for key, name in zip(km, NAMES, strict=True):
        drawn[f"m_{name}"] = 0.1 * jax.random.normal(key, SHAPES[name], jnp.float32)
    for key, name in zip(kv, NAMES, strict=True):
        drawn[f"v_{name}"] = jax.random.uniform(key, SHAPES[name], jnp.float32, 0.005, 0.015)
    return drawn


def matmul(a, w):
    return jnp.dot(a, w, preferred_element_type=jnp.float32).astype(jnp.bfloat16)


def normed(h):
    wide = h.astype(jnp.float32)
    scale = lax.rsqrt(jnp.mean(wide**2, -1, keepdims=True) + 1e-6)
    return (wide * scale).astype(jnp.bfloat16)


def layer(h, w):
    a = normed(h)
    gate = jnp.dot(a, w["w_gate"], preferred_element_type=jnp.float32)
    up = jnp.dot(a, w["w_up"], preferred_element_type=jnp.float32)
    return h + matmul((jax.nn.silu(gate) * up).astype(jnp.bfloat16), w["w_down"])


def adamw(w, m, v, g):
    m = 0.9 * m + 0.1 * g
    v = 0.95 * v + 0.05 * g * g
    step = m * lax.rsqrt(v + 1e-8) + 0.1 * w
    return (w - 0.02 * step).astype(jnp.bfloat16), m, v


def clipped(gradients, sum_of_squares, count):
    factor = jnp.minimum(1.0, 0.5 * lax.rsqrt(sum_of_squares / count + 1e-30))
    return [g * factor for g in gradients]


def stack(weights, h):
    return lax.scan(lambda h, w: (layer(h, w), None), h, weights)[0]


def reference(x, dy, w_gate, w_up, w_down, m_w_gate, m_w_up, m_w_down, v_w_gate, v_w_up, v_w_down):
    weights = dict(zip(NAMES, (w_gate, w_up, w_down), strict=True))

    def take(so_far, sequence):
        h, by_y = sequence
        _, back = jax.vjp(lambda w: stack(w, h), weights)
        return jax.tree.map(lambda total, term: total + term.astype(jnp.float32), so_far, back(by_y)[0]), None

    none_yet = {name: jnp.zeros(w.shape, jnp.float32) for name, w in weights.items()}
    by_weights, _ = lax.scan(take, none_yet, (x, dy))
    gradients = [by_weights[name].astype(jnp.bfloat16).astype(jnp.float32) for name in NAMES]
    gradients = clipped(gradients, sum(jnp.sum(g * g) for g in gradients), sum(g.size for g in gradients))
    new = [
        adamw(w.astype(jnp.float32), m, v, g)
        for w, m, v, g in zip((w_gate, w_up, w_down), (m_w_gate, m_w_up, m_w_down), (v_w_gate, v_w_up, v_w_down), gradients, strict=True)
    ]
    return tuple(one[which] for which in range(3) for one in new)
```

```python
import functools

import jax
import jax.numpy as jnp
from jax import lax
from jax.experimental import pallas as pl
from jax.experimental.pallas import tpu as pltpu
from jax.sharding import PartitionSpec as P

f32, bf16 = jnp.float32, jnp.bfloat16
MESH = pl.DeviceIdType.MESH
FC = 256
SLOTS = 4
HELD = 7
EARLY = 3
TILE = 1024


def dot(a, b):
    return jnp.dot(a, b, preferred_element_type=f32)


def dot_nt(a, b):
    return lax.dot_general(a, b, (((1,), (1,)), ((), ())), preferred_element_type=f32)


def sigmoid(x):
    return 0.5 * jnp.tanh(0.5 * x) + 0.5


def loop(n, body):
    lax.fori_loop(0, n, lambda i, c: (body(i), c)[1], 0)


def train_kernel(n, rounds, x, dy, wg_h, wu_h, wd_h, G, L0, L1, sq_out, A0, A1, AT, H, DY, DYT, ACC, HID, DGU, WGU, WD, PART, RECV, SQ, SQA,
                 in_sem, w_sem, rs_s, rs_r, ag_s, ag_r, own_sem, sq_s, sq_r):
    _, tokens, d = x.shape
    layers, _, ff = wg_h.shape
    chunks = ff // FC
    units = layers * chunks
    last = (L0, L1)
    rows_p, rows_d = d // (2 * n), FC // (2 * n)
    me, rep = lax.axis_index("dp"), lax.axis_index("rep")
    to = (lax.rem(me + 1, n), lax.rem(me + n - 1, n))
    sign = (-1, 1)
    step_rows = tokens // 4

    bar = pltpu.get_barrier_semaphore()
    for k in range(1, n):
        pl.semaphore_signal(bar, inc=1, device_id=(rep, lax.rem(me + k, n)), device_id_type=MESH)

    def w_copies(i):
        slot = lax.rem(i, SLOTS)
        ly = jnp.where(i // chunks == 1, layers - 1, 0)
        c = pl.ds(pl.multiple_of(lax.rem(i, chunks) * FC, FC), FC)
        return (
            pltpu.make_async_copy(wg_h.at[ly, :, c], WGU.at[slot, :, 0:FC], w_sem.at[slot, 0]),
            pltpu.make_async_copy(wu_h.at[ly, :, c], WGU.at[slot, :, FC : 2 * FC], w_sem.at[slot, 1]),
            pltpu.make_async_copy(wd_h.at[ly, c, :], WD.at[slot], w_sem.at[slot, 2]),
        )

    def w_start(i):
        for c in w_copies(i):
            c.start()

    def w_wait(i):
        for c in w_copies(i):
            c.wait()

    x_in = pltpu.make_async_copy(x.at[0], H, in_sem.at[0])
    dy_in = pltpu.make_async_copy(dy.at[0], DY, in_sem.at[1])
    x_in.start()
    w_start(0)
    w_start(1)
    dy_in.start()

    def rows(t):
        return pl.ds(pl.multiple_of(t * step_rows, step_rows), step_rows)

    def scale_of(w):
        return lax.rsqrt(jnp.mean(w * w, -1, keepdims=True) + 1e-6)

    x_in.wait()

    def norm_x(t):
        w = H[rows(t), :].astype(f32)
        A0[rows(t), :] = (w * scale_of(w)).astype(bf16)

    loop(4, norm_x)
    ACC[...] = jnp.zeros_like(ACC)

    def forward(i):
        w_wait(2 * i)
        w_wait(2 * i + 1)
        w_start(2 * i + 2)
        w_start(2 * i + 3)
        total = None
        for k in range(2):
            slot = lax.rem(2 * i + k, SLOTS)
            gu = dot(A0[...], WGU[slot])
            g, u = gu[:, :FC], gu[:, FC:]
            part = dot((g * sigmoid(g) * u).astype(bf16), WD[slot])
            total = part if total is None else total + part
        ACC[...] += total

    loop(chunks // 2, forward)
    dy_in.wait()

    def between(t):
        r = rows(t)
        h = (H[r, :].astype(f32) + ACC[r, :].astype(bf16).astype(f32)).astype(bf16)
        H[r, :] = h
        w = h.astype(f32)
        a = (w * scale_of(w)).astype(bf16)
        A1[r, :] = a
        AT[:, r] = a.T
        DYT[:, r] = DY[r, :].T
        ACC[r, :] = jnp.zeros((step_rows, d), f32)

    loop(4, between)
    pl.semaphore_wait(bar, n - 1)

    def piece(s, h):
        return 2 * lax.rem(me + sign[h] * (1 + s) + 2 * n, n) + h

    def rs_copy(u, s, h):
        return pltpu.make_async_remote_copy(PART.at[u, piece(s, h)], RECV.at[u, s, h], rs_s.at[u, s, h], rs_r.at[u, s, h],
                                            device_id=(rep, to[h]), device_id_type=MESH)

    def rs_take(u, s, h):
        rs_copy(u, s, h).wait_recv()
        p = piece(s + 1, h)
        total = (PART[u, p].astype(f32) + RECV[u, s, h].astype(f32)).astype(bf16)
        PART[u, p] = total
        return total

    def rs_event(u, s):
        @pl.when(s < n - 1)
        def _():
            for h in (0, 1):
                rs_take(u, s - 1, h)
            for h in (0, 1):
                rs_copy(u, s, h).start()

        @pl.when(s == n - 1)
        def _():
            for h in (0, 1):
                g = rs_take(u, n - 2, h).astype(f32)
                SQ[...] += g * g
                own_copy(u, h).start()

    def own_copy(u, h):
        return pltpu.make_async_copy(PART.at[u, 2 * me + h], G.at[h, 0, u], own_sem.at[u, h])

    def done(u, i):
        return jnp.where(i <= EARLY, 2 * (i - u) + 1, (i - u) + 1 + jnp.maximum(EARLY - u, 0))

    def events(i, second, lo, hi):
        def one(q):
            u = i - hi + q
            s = done(u, i - 1) + second

            @pl.when((u >= 0) & (u < units) & (s < n) & (s < done(u, i)))
            def _():
                rs_event(u, s)

        loop(hi - lo + 1, one)

    def backward(ly, A, i):
        w_wait(i + chunks)

        @pl.when(i + 2 < units)
        def _():
            w_start(i + chunks + 2)

        slot = lax.rem(i + chunks, SLOTS)
        wgu, wd = WGU.at[slot], WD.at[slot]

        def tile(t):
            r = pl.ds(pl.multiple_of(t * TILE, TILE), TILE)
            gu = dot(A[r, :], wgu[...])
            g, u = gu[:, :FC], gu[:, FC:]
            by_hid = dot_nt(DY[r, :], wd[...]).astype(bf16).astype(f32)
            sg = sigmoid(g)
            sl = g * sg
            HID[r, :] = (sl * u).astype(bf16)
            DGU[r, FC : 2 * FC] = (by_hid * sl).astype(bf16)
            DGU[r, 0:FC] = (by_hid * u * (sg + sl * (1 - sg))).astype(bf16)

        loop(tokens // TILE, tile)
        events(i, 0, 4, 7)
        wdt = dot(DYT[...], HID[...]).astype(bf16).T
        for k in range(d // FC):
            PART[i, :, 2 * rows_p + k * rows_d : 2 * rows_p + (k + 1) * rows_d] = wdt[:, k * FC : (k + 1) * FC].reshape(2 * n, rows_d, FC)
        events(i, 0, 1, 3)
        gw = dot(AT[...], DGU[...]).astype(bf16)
        PART[i, :, 0:rows_p] = gw[:, :FC].reshape(2 * n, rows_p, FC)
        PART[i, :, rows_p : 2 * rows_p] = gw[:, FC:].reshape(2 * n, rows_p, FC)

        for h in (0, 1):
            rs_copy(i, 0, h).start()
        if ly:
            ACC[...] += dot_nt(DGU[...], wgu[...])
            events(i, 1, 1, 3)

    SQ[...] = jnp.zeros_like(SQ)
    loop(chunks, functools.partial(backward, 1, A1))

    def by_input(t):
        r = rows(t)
        w, da = H[r, :].astype(f32), ACC[r, :].astype(bf16).astype(f32)
        s = scale_of(w)
        along = jnp.sum(da * w, -1, keepdims=True) * (s * s * s) * (1.0 / d)
        by_h = (DY[r, :].astype(f32) + (da * s - w * along).astype(bf16).astype(f32)).astype(bf16)
        DY[r, :] = by_h
        DYT[:, r] = by_h.T
        AT[:, r] = A0[r, :].T

    loop(4, by_input)
    loop(chunks, lambda i: backward(0, A0, i + chunks))

    def ag_copy(u, j, h, dst):
        src = PART.at[u, 2 * me + h] if isinstance(j, int) and j == 0 else G.at[h, j, u]
        return pltpu.make_async_remote_copy(src, dst, ag_s.at[u, j, h], ag_r.at[u, j, h], device_id=(rep, to[h]), device_id_type=MESH)

    per = -(-units // (n - 1))

    def drain(i):
        def one(q):
            u = units + i - n + 1 + q
            s = n - 1 - q

            @pl.when(u < units)
            def _():
                rs_event(u, s)

        loop(n - 1, one)

        def first(k):
            u = i * per + k

            @pl.when(u < units)
            def _():
                for h in (0, 1):
                    ag_copy(u, 0, h, G.at[h, 1, u]).start()

        loop(per, first)

    loop(n - 1, drain)

    lanes = SQA.shape[-1]
    q = SQ[...]
    q = sum(q[:, k * lanes : (k + 1) * lanes] for k in range(FC // lanes))
    SQA[me] = q.reshape(-1, 8, lanes).sum(0)

    def sq_copy(k, slot):
        return pltpu.make_async_remote_copy(SQA.at[me], SQA.at[me], sq_s.at[k], sq_r.at[k], device_id=(rep, lax.rem(me + k, n)), device_id_type=MESH)

    for k in range(1, n):
        sq_copy(k, None).start()

    def gather(t):
        j, u = t // units, lax.rem(t, units)
        for h in (0, 1):
            ag_copy(u, j, h, G.at[h, j + 1, u]).wait_recv()
            ag_copy(u, j + 1, h, G.at[h, j + 2, u]).start()

    loop((rounds - 2) * units, gather)

    def gather_last(u):
        for h in (0, 1):
            ag_copy(u, rounds - 2, h, G.at[h, rounds - 1, u]).wait_recv()
            ag_copy(u, rounds - 1, h, last[h].at[u]).start()

    loop(units, gather_last)

    def sq_from(k):
        src = lax.rem(me + n - k, n)
        return pltpu.make_async_remote_copy(SQA.at[src], SQA.at[src], sq_s.at[k], sq_r.at[k], device_id=(rep, lax.rem(me + k, n)), device_id_type=MESH)

    for k in range(1, n):
        sq_from(k).wait_recv()
    total = SQA[0]
    for k in range(1, n):
        total = total + SQA[k]
    sq_out[...] = jnp.broadcast_to(jnp.sum(total, keepdims=True), sq_out.shape)

    def finish(u):
        for h in (0, 1):
            ag_copy(u, rounds - 1, h, last[h].at[u]).wait_recv()
            own_copy(u, h).wait()

        def sends(s):
            for h in (0, 1):
                rs_copy(u, s, h).wait_send()

        loop(n - 1, sends)

        def sends2(j):
            for h in (0, 1):
                ag_copy(u, j, h, G.at[h, 1, u]).wait_send()

        loop(rounds, sends2)

    loop(units, finish)
    for k in range(1, n):
        sq_copy(k, None).wait_send()


def train(n, rounds, x, dy, w_gate, w_up, w_down):
    _, tokens, d = x.shape
    layers, _, ff = w_gate.shape
    units, rows = layers * ff // FC, 3 * d // (2 * n)
    part = (rows, FC)
    any_ = pl.BlockSpec(memory_space=pl.ANY)
    got = jax.ShapeDtypeStruct((units,) + part, bf16)
    act = pltpu.VMEM((tokens, d), bf16)
    act_t = pltpu.VMEM((d, tokens), bf16)
    dma = pltpu.SemaphoreType.DMA
    return pl.pallas_call(
        functools.partial(train_kernel, n, rounds),
        name="train",
        out_shape=(jax.ShapeDtypeStruct((2, rounds, units) + part, bf16), got, got, jax.ShapeDtypeStruct((8, 128), f32)),
        in_specs=[any_] * 5,
        out_specs=(any_, any_, any_, pl.BlockSpec(memory_space=pltpu.VMEM)),
        scratch_shapes=[
            act, act, act_t, act, act, act_t,
            pltpu.VMEM((tokens, d), f32),
            pltpu.VMEM((tokens, FC), bf16),
            pltpu.VMEM((tokens, 2 * FC), bf16),
            pltpu.VMEM((SLOTS, d, 2 * FC), bf16),
            pltpu.VMEM((SLOTS, FC, d), bf16),
            pltpu.VMEM((units, 2 * n) + part, bf16),
            pltpu.VMEM((units, n - 1, 2) + part, bf16),
            pltpu.VMEM(part, f32),
            pltpu.VMEM((n, 8, 128), f32),
            dma((2,)), dma((SLOTS, 3)),
            dma((units, n - 1, 2)), dma((units, n - 1, 2)),
            dma((units, rounds, 2)), dma((units, rounds, 2)),
            dma((units, 2)), dma((n,)), dma((n,)),
        ],
        compiler_params=pltpu.CompilerParams(collective_id=0, has_side_effects=True, vmem_limit_bytes=67043328),
        cost_estimate=pl.CostEstimate(flops=17 * 2 * tokens * d * ff, bytes_accessed=8 * units * n * rows * FC, transcendentals=0),
    )(x, dy, w_gate, w_up, w_down)


def adam_kernel(n_src, count, source, aliased, index, sq, *refs):
    gs, refs = refs[:n_src], refs[n_src:]
    w, m, v = refs[0:3], refs[3:6], refs[6:9]
    outs = refs[9 + (9 if aliased else 0) :]
    i = pl.program_id(0)
    factor = jnp.minimum(1.0, 0.5 * lax.rsqrt(sq[0:1, 0:1] / count + 1e-30))

    def update(g, k, at):
        g = g.astype(f32) * factor
        new_m = 0.9 * m[k][at] + 0.1 * g
        new_v = 0.95 * v[k][at] + 0.05 * g * g
        old = w[k][at].astype(f32)
        outs[k][at] = (old - 0.02 * (new_m * lax.rsqrt(new_v + 1e-8) + 0.1 * old)).astype(bf16)
        outs[3 + k][at] = new_m
        outs[6 + k][at] = new_v

    def run(g):
        rows_p, rows_d, d = w[0].shape[2], w[2].shape[3], w[2].shape[4]
        for c in range(w[2].shape[1]):
            cols = slice(c * FC, (c + 1) * FC)
            for k in range(2):
                update(g[c, k * rows_p : (k + 1) * rows_p], k, (0, 0, slice(None), cols))
            for k in range(d // FC):
                at = 2 * rows_p + k * rows_d
                update(g[c, at : at + rows_d], 2, (0, c, 0, slice(None), slice(k * FC, (k + 1) * FC)))

    if n_src == 1:
        run(gs[0].at[0, 0] if len(gs[0].shape) == 5 else gs[0])
    else:
        for k in range(n_src):
            pl.when(source(i) == k)(functools.partial(run, gs[k]))


def adam(views, prev, sq, gs, pieces, count, held=None):
    w, m, v = views
    layers, parts, rows_p, ff = w[0].shape
    _, chunks, _, rows_d, d = w[2].shape
    steps = 2 * (held[1] if held else 1)

    wide = pl.BlockSpec((1, 1, rows_p, ff), lambda i, ly, index: (ly, index[i], 0, 0))
    tall = pl.BlockSpec((1, chunks, 1, rows_d, d), lambda i, ly, index: (ly, 0, index[i], 0, 0))
    blocks = [wide, wide, tall]
    rows = gs[0].shape[-2]
    if held:
        g_specs = [pl.BlockSpec((1, 1, chunks, rows, FC), lambda i, ly, index: (lax.rem(i, 2), held[0] + i // 2, layers - 1 - ly, 0, 0))]
    else:
        g_specs = [
            pl.BlockSpec((chunks, rows, FC), lambda i, ly, index: (jnp.where(i == 0, layers - 1 - ly, 0), 0, 0)),
            pl.BlockSpec((chunks, rows, FC), lambda i, ly, index: (jnp.where(i == 1, layers - 1 - ly, layers - 1), 0, 0)),
        ]
    args = [*gs, *w, *m, *v]
    specs = g_specs + blocks * 3
    aliases = {}
    if prev is not None:
        aliases = {2 + len(args) + k: k for k in range(9)}
        args += list(prev)
        specs += [pl.BlockSpec(memory_space=pl.ANY)] * 9
    outs = [jax.ShapeDtypeStruct(a.shape, a.dtype) for a in (*w, *m, *v)]
    moved = 2 * steps * sum(a.size * a.dtype.itemsize for a in (*w, *m, *v)) // parts
    return pl.pallas_call(
        functools.partial(adam_kernel, len(gs), count, lambda i: i, prev is not None),
        name="adam",
        grid_spec=pltpu.PrefetchScalarGridSpec(
            num_scalar_prefetch=1,
            grid=(steps, layers),
            in_specs=[pl.BlockSpec((8, 128), lambda i, ly, index: (0, 0))] + specs,
            out_specs=blocks * 3,
        ),
        out_shape=outs,
        input_output_aliases=aliases,
        compiler_params=pltpu.CompilerParams(vmem_limit_bytes=40 << 20),
        cost_estimate=pl.CostEstimate(flops=30 * moved, bytes_accessed=moved, transcendentals=0),
    )(pieces, sq, *args)


def solution(mesh):
    n = mesh.shape["dp"]

    def step(x, dy, *arrays):
        w = arrays[0:3]
        layers, d, ff = w[0].shape
        count = 3 * w[0].size
        rounds = HELD
        G, *got, sq = train(n, rounds, x, dy, *w)

        def view(a):
            a = list(a)
            for k in range(2):
                a[k] = a[k].reshape(layers, 2 * n, d // (2 * n), ff)
            a[2] = a[2].reshape(layers, ff // FC, 2 * n, FC // (2 * n), d)
            return a

        views = tuple(view(arrays[k : k + 3]) for k in (0, 3, 6))
        me = lax.axis_index("dp")

        def pieces(first, number):
            j = first + jnp.arange(number)
            return jnp.stack([2 * ((me - j + n) % n), 2 * ((me + j) % n) + 1], 1).reshape(-1).astype(jnp.int32)

        right, left = [(k, (k + 1) % n) for k in range(n)], [(k, (k - 1) % n) for k in range(n)]
        out = adam(views, None, sq, [G], pieces(0, rounds), count, (0, rounds))
        for j in range(rounds, n):
            out = adam(views, out, sq, got, pieces(j, 1), count)
            if j < n - 1:
                got = [lax.ppermute(got[0], "dp", right), lax.ppermute(got[1], "dp", left)]
        return tuple(o.reshape(a.shape) for o, a in zip(out, arrays, strict=True))

    return jax.shard_map(
        step,
        mesh=mesh,
        in_specs=(P(("rep", "dp"), None, None),) * 2 + (P(None, None, None),) * 9,
        out_specs=(P("rep", None, None),) * 9,
        check_vma=False,
    )
```

```python
import functools

import jax
import jax.numpy as jnp
from jax import lax
from jax.experimental import pallas as pl
from jax.experimental.pallas import tpu as pltpu
from jax.sharding import PartitionSpec as P


f32, bf16 = jnp.float32, jnp.bfloat16
MESH = pl.DeviceIdType.MESH
FC = 256
SLOTS = 4
HELD = 4
EARLY = 3
TILE = 1024


def dot(a, b):
    return jnp.dot(a, b, preferred_element_type=f32)


def dot_nt(a, b):
    return lax.dot_general(a, b, (((1,), (1,)), ((), ())), preferred_element_type=f32)


def sigmoid(x):
    return 0.5 * jnp.tanh(0.5 * x) + 0.5


def loop(n, body):
    lax.fori_loop(0, n, lambda i, c: (body(i), c)[1], 0)


def train_kernel(n, rounds, x, dy, wg_h, wu_h, wd_h, G, L0, L1, sq_out, A0, A1, AT, H, DY, DYT, ACC, HID, DGU, WGU, WD, PART, RECV, SQ, SQA,
                 in_sem, w_sem, rs_s, rs_r, ag_s, ag_r, own_sem, sq_s, sq_r):
    _, tokens, d = x.shape
    layers, _, ff = wg_h.shape
    chunks = ff // FC
    units = layers * chunks
    last = (L0, L1)
    rows_p, rows_d = d // (2 * n), FC // (2 * n)
    me, rep = lax.axis_index("dp"), lax.axis_index("rep")
    to = (lax.rem(me + 1, n), lax.rem(me + n - 1, n))
    sign = (-1, 1)
    step_rows = tokens // 4

    bar = pltpu.get_barrier_semaphore()
    for k in range(1, n):
        pl.semaphore_signal(bar, inc=1, device_id=(rep, lax.rem(me + k, n)), device_id_type=MESH)

    def w_copies(i):
        slot = lax.rem(i, SLOTS)
        ly = jnp.where(i // chunks == 1, layers - 1, 0)
        c = pl.ds(pl.multiple_of(lax.rem(i, chunks) * FC, FC), FC)
        return (
            pltpu.make_async_copy(wg_h.at[ly, :, c], WGU.at[slot, :, 0:FC], w_sem.at[slot, 0]),
            pltpu.make_async_copy(wu_h.at[ly, :, c], WGU.at[slot, :, FC : 2 * FC], w_sem.at[slot, 1]),
            pltpu.make_async_copy(wd_h.at[ly, c, :], WD.at[slot], w_sem.at[slot, 2]),
        )

    def w_start(i):
        for c in w_copies(i):
            c.start()

    def w_wait(i):
        for c in w_copies(i):
            c.wait()

    x_in = pltpu.make_async_copy(x.at[0], H, in_sem.at[0])
    dy_in = pltpu.make_async_copy(dy.at[0], DY, in_sem.at[1])
    x_in.start()
    w_start(0)
    w_start(1)
    dy_in.start()

    def rows(t):
        return pl.ds(pl.multiple_of(t * step_rows, step_rows), step_rows)

    def scale_of(w):
        return lax.rsqrt(jnp.mean(w * w, -1, keepdims=True) + 1e-6)

    x_in.wait()

    def norm_x(t):
        w = H[rows(t), :].astype(f32)
        A0[rows(t), :] = (w * scale_of(w)).astype(bf16)

    loop(4, norm_x)
    ACC[...] = jnp.zeros_like(ACC)

    def forward(i):
        w_wait(2 * i)
        w_wait(2 * i + 1)
        w_start(2 * i + 2)
        w_start(2 * i + 3)
        total = None
        for k in range(2):
            slot = lax.rem(2 * i + k, SLOTS)
            gu = dot(A0[...], WGU[slot])
            g, u = gu[:, :FC], gu[:, FC:]
            part = dot((g * sigmoid(g) * u).astype(bf16), WD[slot])
            total = part if total is None else total + part
        ACC[...] += total

    loop(chunks // 2, forward)
    dy_in.wait()

    def between(t):
        r = rows(t)
        h = (H[r, :].astype(f32) + ACC[r, :].astype(bf16).astype(f32)).astype(bf16)
        H[r, :] = h
        w = h.astype(f32)
        a = (w * scale_of(w)).astype(bf16)
        A1[r, :] = a
        AT[:, r] = a.T
        DYT[:, r] = DY[r, :].T
        ACC[r, :] = jnp.zeros((step_rows, d), f32)

    loop(4, between)
    pl.semaphore_wait(bar, n - 1)

    def piece(s, h):
        return 2 * lax.rem(me + sign[h] * (1 + s) + 2 * n, n) + h

    def rs_copy(u, s, h):
        return pltpu.make_async_remote_copy(PART.at[u, piece(s, h)], RECV.at[u, s, h], rs_s.at[u, s, h], rs_r.at[u, s, h],
                                            device_id=(rep, to[h]), device_id_type=MESH)

    def rs_take(u, s, h):
        rs_copy(u, s, h).wait_recv()
        p = piece(s + 1, h)
        total = (PART[u, p].astype(f32) + RECV[u, s, h].astype(f32)).astype(bf16)
        PART[u, p] = total
        return total

    def rs_event(u, s):
        @pl.when(s < n - 1)
        def _():
            for h in (0, 1):
                rs_take(u, s - 1, h)
            for h in (0, 1):
                rs_copy(u, s, h).start()

        @pl.when(s == n - 1)
        def _():
            for h in (0, 1):
                g = rs_take(u, n - 2, h).astype(f32)
                SQ[...] += g * g
                own_copy(u, h).start()

    def own_copy(u, h):
        return pltpu.make_async_copy(PART.at[u, 2 * me + h], G.at[h, 0, u], own_sem.at[u, h])

    def done(u, i):
        return jnp.where(i <= EARLY, 2 * (i - u) + 1, (i - u) + 1 + jnp.maximum(EARLY - u, 0))

    def events(i, second, lo, hi):
        def one(q):
            u = i - hi + q
            s = done(u, i - 1) + second

            @pl.when((u >= 0) & (u < units) & (s < n) & (s < done(u, i)))
            def _():
                rs_event(u, s)

        loop(hi - lo + 1, one)

    def backward(ly, A, i):
        w_wait(i + chunks)

        @pl.when(i + 2 < units)
        def _():
            w_start(i + chunks + 2)

        slot = lax.rem(i + chunks, SLOTS)
        wgu, wd = WGU.at[slot], WD.at[slot]

        def tile(t):
            r = pl.ds(pl.multiple_of(t * TILE, TILE), TILE)
            gu = dot(A[r, :], wgu[...])
            g, u = gu[:, :FC], gu[:, FC:]
            by_hid = dot_nt(DY[r, :], wd[...]).astype(bf16).astype(f32)
            sg = sigmoid(g)
            sl = g * sg
            HID[r, :] = (sl * u).astype(bf16)
            DGU[r, FC : 2 * FC] = (by_hid * sl).astype(bf16)
            DGU[r, 0:FC] = (by_hid * u * (sg + sl * (1 - sg))).astype(bf16)

        loop(tokens // TILE, tile)
        events(i, 0, 4, 7)
        wdt = dot(DYT[...], HID[...]).astype(bf16).T
        for k in range(d // FC):
            PART[i, :, 2 * rows_p + k * rows_d : 2 * rows_p + (k + 1) * rows_d] = wdt[:, k * FC : (k + 1) * FC].reshape(2 * n, rows_d, FC)
        events(i, 0, 1, 3)
        gw = dot(AT[...], DGU[...]).astype(bf16)
        PART[i, :, 0:rows_p] = gw[:, :FC].reshape(2 * n, rows_p, FC)
        PART[i, :, rows_p : 2 * rows_p] = gw[:, FC:].reshape(2 * n, rows_p, FC)

        for h in (0, 1):
            rs_copy(i, 0, h).start()
        if ly:
            ACC[...] += dot_nt(DGU[...], wgu[...])
            events(i, 1, 1, 3)

    SQ[...] = jnp.zeros_like(SQ)
    loop(chunks, functools.partial(backward, 1, A1))

    def by_input(t):
        r = rows(t)
        w, da = H[r, :].astype(f32), ACC[r, :].astype(bf16).astype(f32)
        s = scale_of(w)
        along = jnp.sum(da * w, -1, keepdims=True) * (s * s * s) * (1.0 / d)
        by_h = (DY[r, :].astype(f32) + (da * s - w * along).astype(bf16).astype(f32)).astype(bf16)
        DY[r, :] = by_h
        DYT[:, r] = by_h.T
        AT[:, r] = A0[r, :].T

    loop(4, by_input)
    loop(chunks, lambda i: backward(0, A0, i + chunks))

    def ag_copy(u, j, h, dst):
        src = PART.at[u, 2 * me + h] if isinstance(j, int) and j == 0 else G.at[h, j, u]
        return pltpu.make_async_remote_copy(src, dst, ag_s.at[u, j, h], ag_r.at[u, j, h], device_id=(rep, to[h]), device_id_type=MESH)

    per = -(-units // (n - 1))

    def drain(i):
        def one(q):
            u = units + i - n + 1 + q
            s = n - 1 - q

            @pl.when(u < units)
            def _():
                rs_event(u, s)

        loop(n - 1, one)

        def first(k):
            u = i * per + k

            @pl.when(u < units)
            def _():
                for h in (0, 1):
                    ag_copy(u, 0, h, G.at[h, 1, u]).start()

        loop(per, first)

    loop(n - 1, drain)

    lanes = SQA.shape[-1]
    q = SQ[...]
    q = sum(q[:, k * lanes : (k + 1) * lanes] for k in range(FC // lanes))
    SQA[me] = q.reshape(-1, 8, lanes).sum(0)

    def sq_copy(k):
        return pltpu.make_async_remote_copy(SQA.at[me], SQA.at[me], sq_s.at[k], sq_r.at[k], device_id=(rep, lax.rem(me + k, n)), device_id_type=MESH)

    for k in range(1, n):
        sq_copy(k).start()

    def gather(t):
        j, u = t // units, lax.rem(t, units)
        for h in (0, 1):
            ag_copy(u, j, h, G.at[h, j + 1, u]).wait_recv()
            ag_copy(u, j + 1, h, G.at[h, j + 2, u]).start()

    loop((rounds - 2) * units, gather)

    def gather_last(u):
        for h in (0, 1):
            ag_copy(u, rounds - 2, h, G.at[h, rounds - 1, u]).wait_recv()
            ag_copy(u, rounds - 1, h, last[h].at[u]).start()

    loop(units, gather_last)

    def sq_from(k):
        src = lax.rem(me + n - k, n)
        return pltpu.make_async_remote_copy(SQA.at[src], SQA.at[src], sq_s.at[k], sq_r.at[k], device_id=(rep, lax.rem(me + k, n)), device_id_type=MESH)

    for k in range(1, n):
        sq_from(k).wait_recv()
    total = SQA[0]
    for k in range(1, n):
        total = total + SQA[k]
    sq_out[...] = jnp.broadcast_to(jnp.sum(total, keepdims=True), sq_out.shape)

    def finish(u):
        for h in (0, 1):
            ag_copy(u, rounds - 1, h, last[h].at[u]).wait_recv()
            own_copy(u, h).wait()

        def sends(s):
            for h in (0, 1):
                rs_copy(u, s, h).wait_send()

        loop(n - 1, sends)

        def sends2(j):
            for h in (0, 1):
                ag_copy(u, j, h, G.at[h, 1, u]).wait_send()

        loop(rounds, sends2)

    loop(units, finish)
    for k in range(1, n):
        sq_copy(k).wait_send()


def train(n, rounds, x, dy, w_gate, w_up, w_down):
    _, tokens, d = x.shape
    layers, _, ff = w_gate.shape
    units, rows = layers * ff // FC, 3 * d // (2 * n)
    part = (rows, FC)
    any_ = pl.BlockSpec(memory_space=pl.ANY)
    got = jax.ShapeDtypeStruct((units,) + part, bf16)
    act = pltpu.VMEM((tokens, d), bf16)
    act_t = pltpu.VMEM((d, tokens), bf16)
    dma = pltpu.SemaphoreType.DMA
    return pl.pallas_call(
        functools.partial(train_kernel, n, rounds),
        name="train",
        out_shape=(jax.ShapeDtypeStruct((2, rounds, units) + part, bf16), got, got, jax.ShapeDtypeStruct((8, 128), f32)),
        in_specs=[any_] * 5,
        out_specs=(any_, any_, any_, pl.BlockSpec(memory_space=pltpu.VMEM)),
        scratch_shapes=[
            act, act, act_t, act, act, act_t,
            pltpu.VMEM((tokens, d), f32),
            pltpu.VMEM((tokens, FC), bf16),
            pltpu.VMEM((tokens, 2 * FC), bf16),
            pltpu.VMEM((SLOTS, d, 2 * FC), bf16),
            pltpu.VMEM((SLOTS, FC, d), bf16),
            pltpu.VMEM((units, 2 * n) + part, bf16),
            pltpu.VMEM((units, n - 1, 2) + part, bf16),
            pltpu.VMEM(part, f32),
            pltpu.VMEM((n, 8, 128), f32),
            dma((2,)), dma((SLOTS, 3)),
            dma((units, n - 1, 2)), dma((units, n - 1, 2)),
            dma((units, rounds, 2)), dma((units, rounds, 2)),
            dma((units, 2)), dma((n,)), dma((n,)),
        ],
        compiler_params=pltpu.CompilerParams(collective_id=0, has_side_effects=True, vmem_limit_bytes=67043328),
        cost_estimate=pl.CostEstimate(flops=17 * 2 * tokens * d * ff, bytes_accessed=8 * units * n * rows * FC, transcendentals=0),
    )(x, dy, w_gate, w_up, w_down)


def adam_kernel(n_src, count, sources, aliased, index, sq, *refs):
    gs, refs = refs[:n_src], refs[n_src:]
    w, m, v = refs[0:3], refs[3:6], refs[6:9]
    outs = refs[9 + (9 if aliased else 0) :]
    i = pl.program_id(0)
    factor = jnp.minimum(1.0, 0.5 * lax.rsqrt(sq[0:1, 0:1] / count + 1e-30))

    def update(g, k, at):
        g = g.astype(f32) * factor
        new_m = 0.9 * m[k][at] + 0.1 * g
        new_v = 0.95 * v[k][at] + 0.05 * g * g
        old = w[k][at].astype(f32)
        outs[k][at] = (old - 0.02 * (new_m * lax.rsqrt(new_v + 1e-8) + 0.1 * old)).astype(bf16)
        outs[3 + k][at] = new_m
        outs[6 + k][at] = new_v

    def run(g):
        rows_p, rows_d, d = w[0].shape[2], w[2].shape[3], w[2].shape[4]

        def chunk(c):
            cols = pl.ds(pl.multiple_of(c * FC, FC), FC)
            for k in range(2):
                update(g[c, k * rows_p : (k + 1) * rows_p], k, (0, 0, slice(None), cols))
            for k in range(d // FC):
                at = 2 * rows_p + k * rows_d
                update(g[c, at : at + rows_d], 2, (0, c, 0, slice(None), slice(k * FC, (k + 1) * FC)))

        loop(w[2].shape[1], chunk)

    for k in range(n_src):
        g = gs[k].at[0, 0] if len(gs[k].shape) == 5 else gs[k]
        mine = [sources.index(s) for s in sources if s[0] == k]
        pl.when((i >= mine[0]) & (i <= mine[-1]))(functools.partial(run, g))


def adam(views, prev, sq, gs, sources, me, n, count):
    w, m, v = views
    layers, parts, rows_p, ff = w[0].shape
    _, chunks, _, rows_d, d = w[2].shape
    steps = len(sources)
    index = jnp.stack([2 * ((me + (2 * h - 1) * j + n) % n) + h for _, h, j in sources]).astype(jnp.int32)

    wide = pl.BlockSpec((1, 1, rows_p, ff), lambda i, ly, index: (ly, index[i], 0, 0))
    tall = pl.BlockSpec((1, chunks, 1, rows_d, d), lambda i, ly, index: (ly, 0, index[i], 0, 0))
    blocks = [wide, wide, tall]

    def g_spec(k):
        mine = [t for t in range(steps) if sources[t][0] == k]
        lo, hi = mine[0], mine[-1]

        def place(i, ly):
            return jnp.clip(i, lo, hi), jnp.where(i < lo, layers - 1, jnp.where(i > hi, 0, layers - 1 - ly))

        if len(gs[k].shape) == 3:
            return pl.BlockSpec((chunks, gs[k].shape[1], FC), lambda i, ly, index: (place(i, ly)[1], 0, 0))

        def held(i, ly, index):
            t, at = place(i, ly)
            _, _, j = sources[lo]
            return lax.rem(t - lo, 2), j + (t - lo) // 2, at, 0, 0

        return pl.BlockSpec((1, 1, chunks, gs[k].shape[3], FC), held)

    args = [*gs, *w, *m, *v]
    specs = [g_spec(k) for k in range(len(gs))] + blocks * 3
    aliases = {}
    if prev is not None:
        aliases = {2 + len(args) + k: k for k in range(9)}
        args += list(prev)
        specs += [pl.BlockSpec(memory_space=pl.ANY)] * 9
    outs = [jax.ShapeDtypeStruct(a.shape, a.dtype) for a in (*w, *m, *v)]
    moved = 2 * steps * sum(a.size * a.dtype.itemsize for a in (*w, *m, *v)) // parts
    return pl.pallas_call(
        functools.partial(adam_kernel, len(gs), count, sources, prev is not None),
        name="adam",
        grid_spec=pltpu.PrefetchScalarGridSpec(
            num_scalar_prefetch=1,
            grid=(steps, layers),
            in_specs=[pl.BlockSpec((8, 128), lambda i, ly, index: (0, 0))] + specs,
            out_specs=blocks * 3,
        ),
        out_shape=outs,
        input_output_aliases=aliases,
        compiler_params=pltpu.CompilerParams(vmem_limit_bytes=67043328),
        cost_estimate=pl.CostEstimate(flops=30 * moved, bytes_accessed=moved, transcendentals=0),
    )(index, sq, *args)


def solution(mesh):
    n = mesh.shape["dp"]

    def step(x, dy, *arrays):
        w = arrays[0:3]
        count = 3 * w[0].size
        rounds = HELD
        return whole(n, rounds, count, x, dy, arrays)

    def whole(n, rounds, count, x, dy, arrays):
        w = arrays[0:3]
        layers, d, ff = w[0].shape
        G, *got, sq = train(n, rounds, x, dy, *w)

        def view(a):
            a = list(a)
            for k in range(2):
                a[k] = a[k].reshape(layers, 2 * n, d // (2 * n), ff)
            a[2] = a[2].reshape(layers, ff // FC, 2 * n, FC // (2 * n), d)
            return a

        views = tuple(view(arrays[k : k + 3]) for k in (0, 3, 6))
        me = lax.axis_index("dp")
        right, left = [(k, (k + 1) % n) for k in range(n)], [(k, (k - 1) % n) for k in range(n)]

        out, hops = None, n - 1 - rounds
        first = rounds - 1
        for k in range(hops + 1):
            came = got
            if k < hops:
                r = lax.ppermute(came[0], "dp", right)
                got = [r, lax.ppermute(came[1], "dp", left)]
            if k == 0:
                gs, sources = [G], [(0, h, j) for j in range(first) for h in (0, 1)]
                late = came
            else:
                gs, sources = list(came), [(0, 0, rounds + k), (1, 1, rounds + k)]
            if k == min(1, hops):
                gs += [*late, G]
                sources += [(2, 0, rounds), (3, 1, rounds), (4, 0, first), (4, 1, first)]
            out = adam(views, out, sq, gs, sources, me, n, count)
        return tuple(o.reshape(a.shape) for o, a in zip(out, arrays, strict=True))

    return jax.shard_map(
        step,
        mesh=mesh,
        in_specs=(P(("rep", "dp"), None, None),) * 2 + (P(None, None, None),) * 9,
        out_specs=(P("rep", None, None),) * 9,
        check_vma=False,
    )
```

```python
import functools

import jax
import jax.numpy as jnp
from jax import lax
from jax.experimental import pallas as pl
from jax.experimental.pallas import tpu as pltpu
from jax.sharding import PartitionSpec as P


f32, bf16 = jnp.float32, jnp.bfloat16
MESH = pl.DeviceIdType.MESH
FC = 256
SLOTS = 4
HELD = 4
DEPTH = 6
TILE = 1024


def dot(a, b):
    return jnp.dot(a, b, preferred_element_type=f32)


def dot_nt(a, b):
    return lax.dot_general(a, b, (((1,), (1,)), ((), ())), preferred_element_type=f32)


def sigmoid(x):
    return 0.5 * jnp.tanh(0.5 * x) + 0.5


def loop(n, body):
    lax.fori_loop(0, n, lambda i, c: (body(i), c)[1], 0)


def train_kernel(n, rounds, x, dy, wg_h, wu_h, wd_h, G, L0, L1, sq_out, A0, A1, AT, H, DY, DYT, ACC, HID, DGU, WGU, WD, PART, RECV, SQ, SQA,
                 in_sem, w_sem, rs_s, rs_r, ag_s, ag_r, own_sem, sq_sem):
    _, tokens, d = x.shape
    layers, _, ff = wg_h.shape
    chunks = ff // FC
    units = layers * chunks
    last = (L0, L1)
    rows_p, rows_d = d // (2 * n), FC // (2 * n)
    me, rep = lax.axis_index("dp"), lax.axis_index("rep")
    to = (lax.rem(me + 1, n), lax.rem(me + n - 1, n))
    sign = (-1, 1)
    step_rows = tokens // 4

    bar = pltpu.get_barrier_semaphore()
    for k in range(1, n):
        pl.semaphore_signal(bar, inc=1, device_id=(rep, lax.rem(me + k, n)), device_id_type=MESH)

    def w_copies(i):
        slot = lax.rem(i, SLOTS)
        ly = jnp.where(i // chunks == 1, layers - 1, 0)
        c = pl.ds(pl.multiple_of(lax.rem(i, chunks) * FC, FC), FC)
        half = lax.rem(slot, 2)
        first = i < chunks
        at = jnp.where(first, half, 2 * half) * FC
        gap = jnp.where(first, 2, 1) * FC
        return (
            pltpu.make_async_copy(wg_h.at[ly, :, c], WGU.at[slot // 2, :, pl.ds(pl.multiple_of(at, FC), FC)], w_sem.at[slot, 0]),
            pltpu.make_async_copy(wu_h.at[ly, :, c], WGU.at[slot // 2, :, pl.ds(pl.multiple_of(at + gap, FC), FC)], w_sem.at[slot, 1]),
            pltpu.make_async_copy(wd_h.at[ly, c, :], WD.at[slot], w_sem.at[slot, 2]),
        )

    def w_start(i):
        for c in w_copies(i):
            c.start()

    def w_wait(i):
        for c in w_copies(i):
            c.wait()

    x_in = pltpu.make_async_copy(x.at[0], H, in_sem.at[0])
    dy_in = pltpu.make_async_copy(dy.at[0], DY, in_sem.at[1])
    x_in.start()
    w_start(0)
    w_start(1)
    dy_in.start()

    def rows(t):
        return pl.ds(pl.multiple_of(t * step_rows, step_rows), step_rows)

    def scale_of(w):
        return lax.rsqrt(jnp.mean(w * w, -1, keepdims=True) + 1e-6)

    x_in.wait()

    def norm_x(t):
        w = H[rows(t), :].astype(f32)
        A0[rows(t), :] = (w * scale_of(w)).astype(bf16)

    loop(4, norm_x)
    ACC[...] = jnp.zeros_like(ACC)

    def forward(i):
        w_wait(2 * i)
        w_wait(2 * i + 1)
        w_start(2 * i + 2)
        w_start(2 * i + 3)
        pair = lax.rem(i, SLOTS // 2)
        a = A0[...]
        g = dot(a, WGU[pair, :, 0 : 2 * FC])
        u = dot(a, WGU[pair, :, 2 * FC : 4 * FC])
        ACC[...] += dot((g * sigmoid(g) * u).astype(bf16), WD[pl.ds(2 * pair, 2)].reshape(2 * FC, d))

    loop(chunks // 2, forward)
    dy_in.wait()

    def between(t):
        r = rows(t)
        h = (H[r, :].astype(f32) + ACC[r, :].astype(bf16).astype(f32)).astype(bf16)
        H[r, :] = h
        w = h.astype(f32)
        a = (w * scale_of(w)).astype(bf16)
        A1[r, :] = a
        AT[:, r] = a.T
        DYT[:, r] = DY[r, :].T
        ACC[r, :] = jnp.zeros((step_rows, d), f32)

    loop(4, between)
    pl.semaphore_wait(bar, n - 1)

    def piece(s, h):
        return 2 * lax.rem(me + sign[h] * (1 + s) + 2 * n, n) + h

    def rs_copy(u, s, h):
        return pltpu.make_async_remote_copy(PART.at[u, piece(s, h)], RECV.at[u, s, h], rs_s.at[u], rs_r.at[u, s],
                                            device_id=(rep, to[h]), device_id_type=MESH)

    def whole(ref, sem):
        return pltpu.make_async_copy(ref, ref, sem)

    def rs_take(u, s, h):
        p = piece(s + 1, h)
        total = (PART[u, p].astype(f32) + RECV[u, s, h].astype(f32)).astype(bf16)
        PART[u, p] = total
        return total

    def rs_event(u, s):
        whole(RECV.at[u, s - 1], rs_r.at[u, s - 1]).wait()

        @pl.when(s < n - 1)
        def _():
            for h in (0, 1):
                rs_take(u, s - 1, h)
            for h in (0, 1):
                rs_copy(u, s, h).start()

        @pl.when(s == n - 1)
        def _():
            for h in (0, 1):
                g = rs_take(u, n - 2, h).astype(f32)
                SQ[...] += g * g
                own_copy(u, h).start()

    def own_copy(u, h):
        return pltpu.make_async_copy(PART.at[u, 2 * me + h], G.at[h, 0, u], own_sem.at[0])

    def events(i, back, number):
        def one(q):
            s = back - q

            @pl.when(i >= s)
            def _():
                rs_event(i - s, s)

        loop(number, one)

    def backward(ly, A, i):
        w_wait(i + chunks)

        @pl.when(i + 2 < units)
        def _():
            w_start(i + chunks + 2)

        slot = lax.rem(i + chunks, SLOTS)
        wgu = WGU.at[slot // 2, :, pl.ds(pl.multiple_of(lax.rem(slot, 2) * 2 * FC, 2 * FC), 2 * FC)]
        wd = WD.at[slot]

        def tile(t):
            r = pl.ds(pl.multiple_of(t * TILE, TILE), TILE)
            gu = dot(A[r, :], wgu[...])
            g, u = gu[:, :FC], gu[:, FC:]
            by_hid = dot_nt(DY[r, :], wd[...]).astype(bf16).astype(f32)
            sg = sigmoid(g)
            sl = g * sg
            HID[r, :] = (sl * u).astype(bf16)
            DGU[r, FC : 2 * FC] = (by_hid * sl).astype(bf16)
            DGU[r, 0:FC] = (by_hid * u * (sg + sl * (1 - sg))).astype(bf16)
            events(i, jnp.where(t == 0, n - 1, (n - 2) // 2), jnp.where(t == 0, n // 2, (n - 2) // 2 - 1))

        loop(tokens // TILE, tile)
        wdt = dot(DYT[...], HID[...]).astype(bf16).T
        for k in range(d // FC):
            PART[i, :, 2 * rows_p + k * rows_d : 2 * rows_p + (k + 1) * rows_d] = wdt[:, k * FC : (k + 1) * FC].reshape(2 * n, rows_d, FC)
        events(i, 1, 1)
        gw = dot(AT[...], DGU[...]).astype(bf16)
        PART[i, :, 0:rows_p] = gw[:, :FC].reshape(2 * n, rows_p, FC)
        PART[i, :, rows_p : 2 * rows_p] = gw[:, FC:].reshape(2 * n, rows_p, FC)

        for h in (0, 1):
            rs_copy(i, 0, h).start()
        if ly:
            ACC[...] += dot_nt(DGU[...], wgu[...])

    SQ[...] = jnp.zeros_like(SQ)
    loop(chunks, functools.partial(backward, 1, A1))

    def by_input(t):
        r = rows(t)
        w, da = H[r, :].astype(f32), ACC[r, :].astype(bf16).astype(f32)
        s = scale_of(w)
        along = jnp.sum(da * w, -1, keepdims=True) * (s * s * s) * (1.0 / d)
        by_h = (DY[r, :].astype(f32) + (da * s - w * along).astype(bf16).astype(f32)).astype(bf16)
        DY[r, :] = by_h
        DYT[:, r] = by_h.T
        AT[:, r] = A0[r, :].T

    loop(4, by_input)
    loop(chunks, lambda i: backward(0, A0, i + chunks))

    def ag_copy(u, j, h, dst):
        src = PART.at[u, 2 * me + h] if isinstance(j, int) and j == 0 else G.at[h, j, u]
        return pltpu.make_async_remote_copy(src, dst, ag_s.at[u], ag_r.at[u, j], device_id=(rep, to[h]), device_id_type=MESH)

    per = -(-units // (n - 1))

    def drain(i):
        def one(q):
            u = units + i - n + 1 + q
            s = n - 1 - q

            @pl.when(u < units)
            def _():
                rs_event(u, s)

        loop(n - 1, one)

        def first(k):
            u = i * per + k

            @pl.when(u < units)
            def _():
                for h in (0, 1):
                    ag_copy(u, 0, h, G.at[h, 1, u]).start()

        loop(per, first)

    loop(n - 1, drain)

    lanes = SQA.shape[-1]
    q = SQ[...]
    q = sum(q[:, k * lanes : (k + 1) * lanes] for k in range(FC // lanes))
    SQA[me] = q.reshape(-1, 8, lanes).sum(0)

    def sq_copy(k):
        return pltpu.make_async_remote_copy(SQA.at[me], SQA.at[me], sq_sem.at[0], sq_sem.at[1], device_id=(rep, lax.rem(me + k, n)), device_id_type=MESH)

    for k in range(1, n):
        sq_copy(k).start()

    def gather(t):
        j, u = t // units, lax.rem(t, units)
        whole(RECV.at[u, 0], ag_r.at[u, j]).wait()
        for h in (0, 1):
            ag_copy(u, j + 1, h, G.at[h, j + 2, u]).start()

    loop((rounds - 2) * units, gather)

    def gather_last(u):
        whole(RECV.at[u, 0], ag_r.at[u, rounds - 2]).wait()
        for h in (0, 1):
            ag_copy(u, rounds - 1, h, last[h].at[u]).start()

    loop(units, gather_last)

    whole(SQA.at[1:n], sq_sem.at[1]).wait()
    total = SQA[0]
    for k in range(1, n):
        total = total + SQA[k]
    sq_out[...] = jnp.broadcast_to(jnp.sum(total, keepdims=True), sq_out.shape)

    def finish(u):
        whole(RECV.at[u, 0], ag_r.at[u, rounds - 1]).wait()
        whole(RECV.at[u], rs_s.at[u]).wait()
        whole(RECV.at[u, 0:rounds], ag_s.at[u]).wait()

    loop(units, finish)
    whole(RECV.at[:, 0], own_sem.at[0]).wait()
    whole(SQA.at[1:n], sq_sem.at[0]).wait()


def train(n, rounds, x, dy, w_gate, w_up, w_down):
    _, tokens, d = x.shape
    layers, _, ff = w_gate.shape
    units, rows = layers * ff // FC, 3 * d // (2 * n)
    part = (rows, FC)
    any_ = pl.BlockSpec(memory_space=pl.ANY)
    got = jax.ShapeDtypeStruct((units,) + part, bf16)
    act = pltpu.VMEM((tokens, d), bf16)
    act_t = pltpu.VMEM((d, tokens), bf16)
    dma = pltpu.SemaphoreType.DMA
    return pl.pallas_call(
        functools.partial(train_kernel, n, rounds),
        name="train",
        out_shape=(jax.ShapeDtypeStruct((2, rounds, units) + part, bf16), got, got, jax.ShapeDtypeStruct((8, 128), f32)),
        in_specs=[any_] * 5,
        out_specs=(any_, any_, any_, pl.BlockSpec(memory_space=pltpu.VMEM)),
        scratch_shapes=[
            act, act, act_t, act, act, act_t,
            pltpu.VMEM((tokens, d), f32),
            pltpu.VMEM((tokens, FC), bf16),
            pltpu.VMEM((tokens, 2 * FC), bf16),
            pltpu.VMEM((SLOTS // 2, d, 4 * FC), bf16),
            pltpu.VMEM((SLOTS, FC, d), bf16),
            pltpu.VMEM((units, 2 * n) + part, bf16),
            pltpu.VMEM((units, n - 1, 2) + part, bf16),
            pltpu.VMEM(part, f32),
            pltpu.VMEM((n, 8, 128), f32),
            dma((2,)), dma((SLOTS, 3)),
            dma((units,)), dma((units, n - 1)), dma((units,)), dma((units, rounds)), dma((1,)), dma((2,)),
        ],
        compiler_params=pltpu.CompilerParams(collective_id=0, has_side_effects=True, vmem_limit_bytes=67043328),
        cost_estimate=pl.CostEstimate(flops=17 * 2 * tokens * d * ff, bytes_accessed=8 * units * n * rows * FC, transcendentals=0),
    )(x, dy, w_gate, w_up, w_down)


def adam_kernel(n, count, sources, n_src, aliased, sq, *refs):
    gs, w, m, v = refs[:n_src], refs[n_src : n_src + 3], refs[n_src + 3 : n_src + 6], refs[n_src + 6 : n_src + 9]
    refs = refs[n_src + 9 + (9 if aliased else 0) :]
    outs, g_in, wide, tall, in_sem, out_sem = refs[:9], refs[9], refs[10:13], refs[13:16], refs[16], refs[17]
    layers, _, rows_p, _ = w[0].shape
    _, chunks, _, rows_d, d = w[2].shape
    depth = g_in.shape[0]
    steps = layers * len(sources)
    me = lax.axis_index("dp")
    _, h0, j0 = sources[0]

    def place(k):
        t = 2 * j0 + h0 + k // layers
        h, j = lax.rem(t, 2), t // 2
        return lax.rem(k, layers), 2 * lax.rem(me + (2 * h - 1) * j + n, n) + h

    def state(k, arrays, sem, out):
        ly, p = place(k)
        slot = lax.rem(k, depth)
        for q in range(3):
            for x in range(3):
                here = tall[q].at[slot] if x == 2 else wide[q].at[slot, x]
                there = arrays[3 * q + x].at[ly, :, p] if x == 2 else arrays[3 * q + x].at[ly, p]
                yield pltpu.make_async_copy(*((here, there) if out else (there, here)), sem.at[slot])

    def taken(k):
        return state(k, (*w, *m, *v), in_sem, False)

    def given(k):
        return state(k, outs, out_sem, True)

    def arrived(k, sem, times):
        slots = g_in.at[0:times]
        pltpu.make_async_copy(slots, slots, sem.at[lax.rem(k, depth)]).wait()

    def gradient(k, x, t):
        units = pl.ds((layers - 1 - lax.rem(k, layers)) * chunks, chunks)
        at = gs[x].at[units]
        if len(gs[x].shape) == 5:
            i = k // layers - t
            at = gs[x].at[lax.rem(i, 2), sources[t][2] + i // 2, units]
        slot = lax.rem(k, depth)
        return pltpu.make_async_copy(at, g_in.at[slot], in_sem.at[slot])

    spans = [[t for t, src in enumerate(sources) if src[0] == x] for x in range(n_src)]

    def start(k):
        for c in taken(k):
            c.start()
        for x, span in enumerate(spans):

            @pl.when((k >= layers * span[0]) & (k < layers * (span[-1] + 1)))
            def _():
                gradient(k, x, span[0]).start()

    loop(min(depth - 2, steps), start)
    factor = jnp.minimum(1.0, 0.5 * lax.rsqrt(sq[0:1, 0:1] / count + 1e-30))

    def update(g, rows):
        g = g.astype(f32) * factor
        w, m, v = rows
        new_m = 0.9 * m[...] + 0.1 * g
        new_v = 0.95 * v[...] + 0.05 * g * g
        old = w[...].astype(f32)
        m[...] = new_m
        v[...] = new_v
        w[...] = (old - 0.02 * (new_m * lax.rsqrt(new_v + 1e-8) + 0.1 * old)).astype(bf16)

    def step(k):
        slot = lax.rem(k, depth)
        arrived(k, in_sem, 6)

        def chunk(c):
            cols = pl.ds(pl.multiple_of(c * FC, FC), FC)
            for x in range(2):
                update(g_in[slot, c, x * rows_p : (x + 1) * rows_p], [a.at[slot, x, :, cols] for a in wide])
            for x in range(d // FC):
                at = 2 * rows_p + x * rows_d
                update(g_in[slot, c, at : at + rows_d], [a.at[slot, c, :, x * FC : (x + 1) * FC] for a in tall])

        loop(chunks, chunk)
        for c in given(k):
            c.start()

        @pl.when(k >= 2)
        def _():
            arrived(k - 2, out_sem, 5)

        @pl.when(k + depth - 2 < steps)
        def _():
            start(k + depth - 2)

    loop(steps, step)

    def finish(k):
        arrived(steps - 2 + k, out_sem, 5)

    loop(2, finish)


def adam(views, prev, sq, gs, sources, n, count):
    w, m, v = views
    _, parts, rows_p, ff = w[0].shape
    _, chunks, _, rows_d, d = w[2].shape
    any_ = pl.BlockSpec(memory_space=pl.ANY)
    args = [*gs, *w, *m, *v]
    aliases = {}
    if prev is not None:
        aliases = {1 + len(args) + k: k for k in range(9)}
        args += list(prev)
    moved = 2 * len(sources) * sum(a.size * a.dtype.itemsize for a in (*w, *m, *v)) // parts
    types = (bf16, f32, f32)
    return pl.pallas_call(
        functools.partial(adam_kernel, n, count, sources, len(gs), prev is not None),
        name="adam",
        in_specs=[pl.BlockSpec(memory_space=pltpu.VMEM)] + [any_] * len(args),
        out_specs=[any_] * 9,
        out_shape=[jax.ShapeDtypeStruct(a.shape, a.dtype) for a in (*w, *m, *v)],
        input_output_aliases=aliases,
        scratch_shapes=[pltpu.VMEM((DEPTH, chunks, gs[0].shape[-2], FC), bf16)]
        + [pltpu.VMEM((DEPTH, 2, rows_p, ff), t) for t in types]
        + [pltpu.VMEM((DEPTH, chunks, rows_d, d), t) for t in types]
        + [pltpu.SemaphoreType.DMA((DEPTH,)), pltpu.SemaphoreType.DMA((DEPTH,))],
        compiler_params=pltpu.CompilerParams(vmem_limit_bytes=67043328),
        cost_estimate=pl.CostEstimate(flops=30 * moved, bytes_accessed=moved, transcendentals=0),
    )(sq, *args)


def solution(mesh):
    n = mesh.shape["dp"]

    def step(x, dy, *arrays):
        w = arrays[0:3]
        count = 3 * w[0].size
        rounds = HELD
        return whole(n, rounds, count, x, dy, arrays)

    def whole(n, rounds, count, x, dy, arrays):
        w = arrays[0:3]
        layers, d, ff = w[0].shape
        G, *got, sq = train(n, rounds, x, dy, *w)

        def view(a):
            a = list(a)
            for k in range(2):
                a[k] = a[k].reshape(layers, 2 * n, d // (2 * n), ff)
            a[2] = a[2].reshape(layers, ff // FC, 2 * n, FC // (2 * n), d)
            return a

        views = tuple(view(arrays[k : k + 3]) for k in (0, 3, 6))
        right, left = [(k, (k + 1) % n) for k in range(n)], [(k, (k - 1) % n) for k in range(n)]

        out, hops = None, n - 1 - rounds
        first = rounds - 1
        for k in range(hops + 1):
            came = got
            if k < hops:
                r = lax.ppermute(came[0], "dp", right)
                got = [r, lax.ppermute(came[1], "dp", left)]
            if k == 0:
                gs, sources = [G], [(0, h, j) for j in range(first) for h in (0, 1)]
                late = came
            elif k == 1:
                gs = [G, *late, *came]
                sources = [(0, 0, first), (0, 1, first), (1, 0, rounds), (2, 1, rounds), (3, 0, rounds + 1), (4, 1, rounds + 1)]
            else:
                gs, sources = list(came), [(0, 0, rounds + k), (1, 1, rounds + k)]
            out = adam(views, out, sq, gs, sources, n, count)
        return tuple(o.reshape(a.shape) for o, a in zip(out, arrays, strict=True))

    return jax.shard_map(
        step,
        mesh=mesh,
        in_specs=(P(("rep", "dp"), None, None),) * 2 + (P(None, None, None),) * 9,
        out_specs=(P("rep", None, None),) * 9,
        check_vma=False,
    )
```

```python
import functools

import jax
import jax.numpy as jnp
from jax import lax
from jax.experimental import pallas as pl
from jax.experimental.pallas import tpu as pltpu
from jax.sharding import PartitionSpec as P


f32, bf16 = jnp.float32, jnp.bfloat16
MESH = pl.DeviceIdType.MESH
FC = 256
SLOTS = 4
JOINT = 2
HELD = 3
DEPTH = 6
TILE = 1024


def dot(a, b):
    return jnp.dot(a, b, preferred_element_type=f32)


def dot_nt(a, b):
    return lax.dot_general(a, b, (((1,), (1,)), ((), ())), preferred_element_type=f32)


def sigmoid(x):
    return 0.5 * jnp.tanh(0.5 * x) + 0.5


def loop(n, body):
    lax.fori_loop(0, n, lambda i, c: (body(i), c)[1], 0)


def train_kernel(n, rounds, x, dy, wg_h, wu_h, wd_h, G, L0, L1, sq_out, A0, A1, AT, H, DY, DYT, ACC, HID, DGU, WGU, WD, PART, RECV, SQ, SQA,
                 in_sem, w_sem, rs_s, rs_r, ag_s, ag_r, own_sem, sq_sem):
    _, tokens, d = x.shape
    layers, _, ff = wg_h.shape
    chunks = ff // FC
    units = layers * chunks
    last = (L0, L1)
    rows_p, rows_d = d // (2 * n), FC // (2 * n)
    me, rep = lax.axis_index("dp"), lax.axis_index("rep")
    to = (lax.rem(me + 1, n), lax.rem(me + n - 1, n))
    sign = (-1, 1)
    step_rows = tokens // 4

    bar = pltpu.get_barrier_semaphore()
    for k in range(1, n):
        pl.semaphore_signal(bar, inc=1, device_id=(rep, lax.rem(me + k, n)), device_id_type=MESH)

    def w_copies(i):
        slot = lax.rem(i, SLOTS)
        ly = jnp.where(i // chunks == 1, layers - 1, 0)
        c = pl.ds(pl.multiple_of(lax.rem(i, chunks) * FC, FC), FC)
        half = lax.rem(slot, 2)
        first = i < chunks
        at = jnp.where(first, half, 2 * half) * FC
        gap = jnp.where(first, 2, 1) * FC
        return (
            pltpu.make_async_copy(wg_h.at[ly, :, c], WGU.at[slot // 2, :, pl.ds(pl.multiple_of(at, FC), FC)], w_sem.at[slot, 0]),
            pltpu.make_async_copy(wu_h.at[ly, :, c], WGU.at[slot // 2, :, pl.ds(pl.multiple_of(at + gap, FC), FC)], w_sem.at[slot, 1]),
            pltpu.make_async_copy(wd_h.at[ly, c, :], WD.at[slot], w_sem.at[slot, 2]),
        )

    def w_start(i):
        for c in w_copies(i):
            c.start()

    def w_wait(i):
        for c in w_copies(i):
            c.wait()

    def rows(t):
        return pl.ds(pl.multiple_of(t * step_rows, step_rows), step_rows)

    def x_in(t):
        return pltpu.make_async_copy(x.at[0, rows(t)], H.at[rows(t)], in_sem.at[t])

    dy_in = pltpu.make_async_copy(dy.at[0], DY, in_sem.at[4])
    loop(4, lambda t: x_in(t).start())
    w_start(0)
    w_start(1)
    dy_in.start()

    def scale_of(w):
        return lax.rsqrt(jnp.mean(w * w, -1, keepdims=True) + 1e-6)

    def norm_x(t):
        x_in(t).wait()
        w = H[rows(t), :].astype(f32)
        A0[rows(t), :] = (w * scale_of(w)).astype(bf16)

    loop(4, norm_x)
    ACC[...] = jnp.zeros_like(ACC)

    def forward(i):
        w_wait(2 * i)
        w_wait(2 * i + 1)
        w_start(2 * i + 2)
        w_start(2 * i + 3)
        pair = lax.rem(i, SLOTS // 2)
        a = A0[...]
        g = dot(a, WGU[pair, :, 0 : 2 * FC])
        u = dot(a, WGU[pair, :, 2 * FC : 4 * FC])
        ACC[...] += dot((g * sigmoid(g) * u).astype(bf16), WD[pl.ds(2 * pair, 2)].reshape(2 * FC, d))
        t = rows(lax.rem(i, 4))
        DYT[:, t] = DY[t, :].T

    dy_in.wait()
    loop(chunks // 2, forward)

    def between(t):
        r = rows(t)
        h = (H[r, :].astype(f32) + ACC[r, :].astype(bf16).astype(f32)).astype(bf16)
        H[r, :] = h
        w = h.astype(f32)
        a = (w * scale_of(w)).astype(bf16)
        A1[r, :] = a
        AT[:, r] = a.T
        ACC[r, :] = jnp.zeros((step_rows, d), f32)

    loop(4, between)
    pl.semaphore_wait(bar, n - 1)

    def piece(s, h):
        return 2 * lax.rem(me + sign[h] * (1 + s) + 2 * n, n) + h

    def rs_copy(u, s, h):
        return pltpu.make_async_remote_copy(PART.at[u, piece(s, h)], RECV.at[u, s, h], rs_s.at[u], rs_r.at[u, s],
                                            device_id=(rep, to[h]), device_id_type=MESH)

    def whole(ref, sem):
        return pltpu.make_async_copy(ref, ref, sem)

    def rs_take(u, s, h):
        p = piece(s + 1, h)
        total = (PART[u, p].astype(f32) + RECV[u, s, h].astype(f32)).astype(bf16)
        PART[u, p] = total
        return total

    def rs_event(u, s):
        whole(RECV.at[u, s - 1], rs_r.at[u, s - 1]).wait()

        @pl.when(s < n - 1)
        def _():
            for h in (0, 1):
                rs_take(u, s - 1, h)
            for h in (0, 1):
                rs_copy(u, s, h).start()

        @pl.when(s == n - 1)
        def _():
            for h in (0, 1):
                g = rs_take(u, n - 2, h).astype(f32)
                SQ[...] += g * g
                own_copy(u, h).start()

    def own_copy(u, h):
        return pltpu.make_async_copy(PART.at[u, 2 * me + h], G.at[h, 0, u], own_sem.at[0])

    def events(i, back, number):
        def one(q):
            s = back - q

            @pl.when(i >= s)
            def _():
                rs_event(i - s, s)

        loop(number, one)

    def backward(ly, A, i):
        w_wait(i + chunks)

        @pl.when(i + 2 < units)
        def _():
            w_start(i + chunks + 2)

        slot = lax.rem(i + chunks, SLOTS)
        wgu = WGU.at[slot // 2, :, pl.ds(pl.multiple_of(lax.rem(slot, 2) * 2 * FC, 2 * FC), 2 * FC)]
        wd = WD.at[slot]

        def tile(t):
            r = pl.ds(pl.multiple_of(t * TILE, TILE), TILE)
            gu = dot(A[r, :], wgu[...])
            g, u = gu[:, :FC], gu[:, FC:]
            by_hid = dot_nt(DY[r, :], wd[...]).astype(bf16).astype(f32)
            sg = sigmoid(g)
            sl = g * sg
            HID[r, :] = (sl * u).astype(bf16)
            DGU[r, FC : 2 * FC] = (by_hid * sl).astype(bf16)
            DGU[r, 0:FC] = (by_hid * u * (sg + sl * (1 - sg))).astype(bf16)
            events(i, jnp.where(t == 0, n - 1, (n - 2) // 2), jnp.where(t == 0, n // 2, (n - 2) // 2 - 1))

        loop(tokens // TILE, tile)
        wdt = dot(DYT[...], HID[...]).astype(bf16).T
        for k in range(d // FC):
            PART[i, :, 2 * rows_p + k * rows_d : 2 * rows_p + (k + 1) * rows_d] = wdt[:, k * FC : (k + 1) * FC].reshape(2 * n, rows_d, FC)
        events(i, 1, 1)
        gw = dot(AT[...], DGU[...]).astype(bf16)
        PART[i, :, 0:rows_p] = gw[:, :FC].reshape(2 * n, rows_p, FC)
        PART[i, :, rows_p : 2 * rows_p] = gw[:, FC:].reshape(2 * n, rows_p, FC)

        for h in (0, 1):
            rs_copy(i, 0, h).start()
        if ly:
            ACC[...] += dot_nt(DGU[...], wgu[...])

    SQ[...] = jnp.zeros_like(SQ)
    loop(chunks, functools.partial(backward, 1, A1))

    def by_input(t):
        r = rows(t)
        w, da = H[r, :].astype(f32), ACC[r, :].astype(bf16).astype(f32)
        s = scale_of(w)
        along = jnp.sum(da * w, -1, keepdims=True) * (s * s * s) * (1.0 / d)
        by_h = (DY[r, :].astype(f32) + (da * s - w * along).astype(bf16).astype(f32)).astype(bf16)
        DY[r, :] = by_h
        DYT[:, r] = by_h.T
        AT[:, r] = A0[r, :].T

    loop(4, by_input)
    loop(chunks, lambda i: backward(0, A0, i + chunks))

    groups = units // JOINT

    def ag_copy(g, j, h):
        us = pl.ds(JOINT * g, JOINT)
        src = PART.at[us, 2 * me + h] if isinstance(j, int) and j == 0 else G.at[h, j, us]
        dst = last[h].at[us] if isinstance(j, int) and j == rounds - 1 else G.at[h, j + 1, us]
        return pltpu.make_async_remote_copy(src, dst, ag_s.at[g], ag_r.at[g, j], device_id=(rep, to[h]), device_id_type=MESH)

    def ag_wait(g, j):
        whole(RECV.at[0:JOINT, 0], ag_r.at[g, j]).wait()

    def drain(i):
        def one(q):
            u = units + i - n + 1 + q
            s = n - 1 - q

            @pl.when(u < units)
            def _():
                rs_event(u, s)

        loop(n - 1, one)

        def first(k):
            g = groups * i // (n - 1) + k

            @pl.when(g < groups * (i + 1) // (n - 1))
            def _():
                for h in (0, 1):
                    ag_copy(g, 0, h).start()

        loop(-(-groups // (n - 1)), first)

    loop(n - 1, drain)

    lanes = SQA.shape[-1]
    q = SQ[...]
    q = sum(q[:, k * lanes : (k + 1) * lanes] for k in range(FC // lanes))
    SQA[me] = q.reshape(-1, 8, lanes).sum(0)

    def sq_copy(k):
        return pltpu.make_async_remote_copy(SQA.at[me], SQA.at[me], sq_sem.at[0], sq_sem.at[1], device_id=(rep, lax.rem(me + k, n)), device_id_type=MESH)

    for k in range(1, n):
        sq_copy(k).start()

    def gather(t):
        j, g = t // groups, lax.rem(t, groups)
        ag_wait(g, j)
        for h in (0, 1):
            ag_copy(g, j + 1, h).start()

    loop((rounds - 2) * groups, gather)

    def gather_last(g):
        ag_wait(g, rounds - 2)
        for h in (0, 1):
            ag_copy(g, rounds - 1, h).start()

    loop(groups, gather_last)
    whole(SQA.at[1:n], sq_sem.at[1]).wait()
    total = SQA[0]
    for k in range(1, n):
        total = total + SQA[k]
    sq_out[...] = jnp.broadcast_to(jnp.sum(total, keepdims=True), sq_out.shape)

    def finish(u):
        whole(RECV.at[u], rs_s.at[u]).wait()

    def finish_ag(g):
        ag_wait(g, rounds - 1)
        whole(RECV.at[0:JOINT, 0:rounds], ag_s.at[g]).wait()

    loop(groups, finish_ag)
    loop(units, finish)
    whole(RECV.at[:, 0], own_sem.at[0]).wait()
    whole(SQA.at[1:n], sq_sem.at[0]).wait()


def train(n, rounds, x, dy, w_gate, w_up, w_down):
    _, tokens, d = x.shape
    layers, _, ff = w_gate.shape
    units, rows = layers * ff // FC, 3 * d // (2 * n)
    part = (rows, FC)
    any_ = pl.BlockSpec(memory_space=pl.ANY)
    got = jax.ShapeDtypeStruct((units,) + part, bf16)
    act = pltpu.VMEM((tokens, d), bf16)
    act_t = pltpu.VMEM((d, tokens), bf16)
    dma = pltpu.SemaphoreType.DMA
    return pl.pallas_call(
        functools.partial(train_kernel, n, rounds),
        name="train",
        out_shape=(jax.ShapeDtypeStruct((2, rounds, units) + part, bf16), got, got, jax.ShapeDtypeStruct((8, 128), f32)),
        in_specs=[any_] * 5,
        out_specs=(any_, any_, any_, pl.BlockSpec(memory_space=pltpu.VMEM)),
        scratch_shapes=[
            act, act, act_t, act, act, act_t,
            pltpu.VMEM((tokens, d), f32),
            pltpu.VMEM((tokens, FC), bf16),
            pltpu.VMEM((tokens, 2 * FC), bf16),
            pltpu.VMEM((SLOTS // 2, d, 4 * FC), bf16),
            pltpu.VMEM((SLOTS, FC, d), bf16),
            pltpu.VMEM((units, 2 * n) + part, bf16),
            pltpu.VMEM((units, n - 1, 2) + part, bf16),
            pltpu.VMEM(part, f32),
            pltpu.VMEM((n, 8, 128), f32),
            dma((5,)), dma((SLOTS, 3)),
            dma((units,)), dma((units, n - 1)), dma((units // JOINT,)), dma((units // JOINT, rounds)), dma((1,)), dma((2,)),
        ],
        compiler_params=pltpu.CompilerParams(collective_id=0, has_side_effects=True, vmem_limit_bytes=67043328),
        cost_estimate=pl.CostEstimate(flops=17 * 2 * tokens * d * ff, bytes_accessed=8 * units * n * rows * FC, transcendentals=0),
    )(x, dy, w_gate, w_up, w_down)


def adam_kernel(n, count, sources, n_src, aliased, sq, *refs):
    gs, w, m, v = refs[:n_src], refs[n_src : n_src + 3], refs[n_src + 3 : n_src + 6], refs[n_src + 6 : n_src + 9]
    refs = refs[n_src + 9 + (9 if aliased else 0) :]
    outs, g_in, wide, tall, in_sem, out_sem = refs[:9], refs[9], refs[10:13], refs[13:16], refs[16], refs[17]
    layers, _, rows_p, _ = w[0].shape
    _, chunks, _, rows_d, d = w[2].shape
    depth = g_in.shape[0]
    steps = layers * len(sources)
    me = lax.axis_index("dp")
    _, h0, j0 = sources[0]

    def place(k):
        t = 2 * j0 + h0 + k // layers
        h, j = lax.rem(t, 2), t // 2
        return lax.rem(k, layers), 2 * lax.rem(me + (2 * h - 1) * j + n, n) + h

    def state(k, arrays, sem, out):
        ly, p = place(k)
        slot = lax.rem(k, depth)
        for q in range(3):
            for x in range(3):
                here = tall[q].at[slot] if x == 2 else wide[q].at[slot, x]
                there = arrays[3 * q + x].at[ly, :, p] if x == 2 else arrays[3 * q + x].at[ly, p]
                yield pltpu.make_async_copy(*((here, there) if out else (there, here)), sem.at[slot])

    def taken(k):
        return state(k, (*w, *m, *v), in_sem, False)

    def given(k):
        return state(k, outs, out_sem, True)

    def arrived(k, sem, times):
        slots = g_in.at[0:times]
        pltpu.make_async_copy(slots, slots, sem.at[lax.rem(k, depth)]).wait()

    def gradient(k, x, t):
        units = pl.ds((layers - 1 - lax.rem(k, layers)) * chunks, chunks)
        at = gs[x].at[units]
        if len(gs[x].shape) == 5:
            i = 2 * sources[t][2] + sources[t][1] + k // layers - t
            at = gs[x].at[lax.rem(i, 2), i // 2, units]
        slot = lax.rem(k, depth)
        return pltpu.make_async_copy(at, g_in.at[slot], in_sem.at[slot])

    spans = [[t for t, src in enumerate(sources) if src[0] == x] for x in range(n_src)]

    def start(k):
        for c in taken(k):
            c.start()
        for x, span in enumerate(spans):

            @pl.when((k >= layers * span[0]) & (k < layers * (span[-1] + 1)))
            def _():
                gradient(k, x, span[0]).start()

    loop(min(depth - 2, steps), start)
    factor = jnp.minimum(1.0, 0.5 * lax.rsqrt(sq[0:1, 0:1] / count + 1e-30))

    def update(g, rows):
        g = g.astype(f32) * factor
        w, m, v = rows
        new_m = 0.9 * m[...] + 0.1 * g
        new_v = 0.95 * v[...] + 0.05 * g * g
        old = w[...].astype(f32)
        m[...] = new_m
        v[...] = new_v
        w[...] = (old - 0.02 * (new_m * lax.rsqrt(new_v + 1e-8) + 0.1 * old)).astype(bf16)

    def step(k):
        slot = lax.rem(k, depth)
        arrived(k, in_sem, 6)

        def chunk(c):
            cols = pl.ds(pl.multiple_of(c * FC, FC), FC)
            for x in range(2):
                update(g_in[slot, c, x * rows_p : (x + 1) * rows_p], [a.at[slot, x, :, cols] for a in wide])
            for x in range(d // FC):
                at = 2 * rows_p + x * rows_d
                update(g_in[slot, c, at : at + rows_d], [a.at[slot, c, :, x * FC : (x + 1) * FC] for a in tall])

        loop(chunks, chunk)
        for c in given(k):
            c.start()

        @pl.when(k >= 2)
        def _():
            arrived(k - 2, out_sem, 5)

        @pl.when(k + depth - 2 < steps)
        def _():
            start(k + depth - 2)

    loop(steps, step)

    def finish(k):
        arrived(steps - 2 + k, out_sem, 5)

    loop(2, finish)


def adam(views, prev, sq, gs, sources, n, count):
    w, m, v = views
    _, parts, rows_p, ff = w[0].shape
    _, chunks, _, rows_d, d = w[2].shape
    any_ = pl.BlockSpec(memory_space=pl.ANY)
    args = [*gs, *w, *m, *v]
    aliases = {}
    if prev is not None:
        aliases = {1 + len(args) + k: k for k in range(9)}
        args += list(prev)
    moved = 2 * len(sources) * sum(a.size * a.dtype.itemsize for a in (*w, *m, *v)) // parts
    types = (bf16, f32, f32)
    return pl.pallas_call(
        functools.partial(adam_kernel, n, count, sources, len(gs), prev is not None),
        name="adam",
        in_specs=[pl.BlockSpec(memory_space=pltpu.VMEM)] + [any_] * len(args),
        out_specs=[any_] * 9,
        out_shape=[jax.ShapeDtypeStruct(a.shape, a.dtype) for a in (*w, *m, *v)],
        input_output_aliases=aliases,
        scratch_shapes=[pltpu.VMEM((DEPTH, chunks, gs[0].shape[-2], FC), bf16)]
        + [pltpu.VMEM((DEPTH, 2, rows_p, ff), t) for t in types]
        + [pltpu.VMEM((DEPTH, chunks, rows_d, d), t) for t in types]
        + [pltpu.SemaphoreType.DMA((DEPTH,)), pltpu.SemaphoreType.DMA((DEPTH,))],
        compiler_params=pltpu.CompilerParams(vmem_limit_bytes=67043328),
        cost_estimate=pl.CostEstimate(flops=30 * moved, bytes_accessed=moved, transcendentals=0),
    )(sq, *args)


def solution(mesh):
    n = mesh.shape["dp"]

    def step(x, dy, *arrays):
        w = arrays[0:3]
        count = 3 * w[0].size
        rounds = HELD
        return whole(n, rounds, count, x, dy, arrays)

    def whole(n, rounds, count, x, dy, arrays):
        w = arrays[0:3]
        layers, d, ff = w[0].shape
        G, *got, sq = train(n, rounds, x, dy, *w)

        def view(a):
            a = list(a)
            for k in range(2):
                a[k] = a[k].reshape(layers, 2 * n, d // (2 * n), ff)
            a[2] = a[2].reshape(layers, ff // FC, 2 * n, FC // (2 * n), d)
            return a

        views = tuple(view(arrays[k : k + 3]) for k in (0, 3, 6))
        right, left = [(k, (k + 1) % n) for k in range(n)], [(k, (k - 1) % n) for k in range(n)]

        out, hops = None, n - 1 - rounds
        came, at = [got], 0
        for k in range(hops + 1):
            if k < hops:
                r = lax.ppermute(came[k][0], "dp", right)
                came.append([r, lax.ppermute(came[k][1], "dp", left)])
            gs, sources = [], []
            for p in range(at, at + (-(-(2 * n - 2 - at) // (hops - k)) if k < hops else 2)):
                j, h = p // 2, p % 2
                g = G if j < rounds else came[j - rounds][h]
                if not any(g is o for o in gs):
                    gs.append(g)
                sources.append((len(gs) - 1, h, j))
            at += len(sources)
            out = adam(views, out, sq, gs, sources, n, count)
        return tuple(o.reshape(a.shape) for o, a in zip(out, arrays, strict=True))

    return jax.shard_map(
        step,
        mesh=mesh,
        in_specs=(P(("rep", "dp"), None, None),) * 2 + (P(None, None, None),) * 9,
        out_specs=(P("rep", None, None),) * 9,
        check_vma=False,
    )
```

```python
import functools

import jax
import jax.numpy as jnp
from jax import lax
from jax.experimental import pallas as pl
from jax.experimental.pallas import tpu as pltpu
from jax.sharding import PartitionSpec as P


f32, bf16 = jnp.float32, jnp.bfloat16
MESH = pl.DeviceIdType.MESH
FC = 256
SLOTS = 4
JOINT = 2
HELD = 3
DEPTH = 6
TILE = 1024


def dot(a, b):
    return jnp.dot(a, b, preferred_element_type=f32)


def dot_nt(a, b):
    return lax.dot_general(a, b, (((1,), (1,)), ((), ())), preferred_element_type=f32)


def sigmoid(x):
    return 0.5 * jnp.tanh(0.5 * x) + 0.5


def loop(n, body):
    lax.fori_loop(0, n, lambda i, c: (body(i), c)[1], 0)


def train_kernel(n, rounds, x, dy, wg_h, wu_h, wd_h, G, L00, L01, L10, L11, sq_out, A0, A1, AT, H, DY, DYT, ACC, HID, DGU, WGU, WD, PART, RECV, SQ, SQA,
                 in_sem, w_sem, rs_s, rs_r, ag_s, ag_r, own_sem, sq_sem):
    _, tokens, d = x.shape
    layers, _, ff = wg_h.shape
    chunks = ff // FC
    units = layers * chunks
    last = ((L00, L01), (L10, L11))
    rows_p, rows_d = d // (2 * n), FC // (2 * n)
    me, rep = lax.axis_index("dp"), lax.axis_index("rep")
    to = (lax.rem(me + 1, n), lax.rem(me + n - 1, n))
    sign = (-1, 1)
    step_rows = tokens // 4

    bar = pltpu.get_barrier_semaphore()
    for k in range(1, n):
        pl.semaphore_signal(bar, inc=1, device_id=(rep, lax.rem(me + k, n)), device_id_type=MESH)

    def w_copies(i):
        slot = lax.rem(i, SLOTS)
        ly = jnp.where(i // chunks == 1, layers - 1, 0)
        c = pl.ds(pl.multiple_of(lax.rem(i, chunks) * FC, FC), FC)
        half = lax.rem(slot, 2)
        first = i < chunks
        at = jnp.where(first, half, 2 * half) * FC
        gap = jnp.where(first, 2, 1) * FC
        return (
            pltpu.make_async_copy(wg_h.at[ly, :, c], WGU.at[slot // 2, :, pl.ds(pl.multiple_of(at, FC), FC)], w_sem.at[slot, 0]),
            pltpu.make_async_copy(wu_h.at[ly, :, c], WGU.at[slot // 2, :, pl.ds(pl.multiple_of(at + gap, FC), FC)], w_sem.at[slot, 1]),
            pltpu.make_async_copy(wd_h.at[ly, c, :], WD.at[slot], w_sem.at[slot, 2]),
        )

    def w_start(i):
        for c in w_copies(i):
            c.start()

    def w_wait(i):
        for c in w_copies(i):
            c.wait()

    def rows(t):
        return pl.ds(pl.multiple_of(t * step_rows, step_rows), step_rows)

    def x_in(t):
        return pltpu.make_async_copy(x.at[0, rows(t)], H.at[rows(t)], in_sem.at[t])

    dy_in = pltpu.make_async_copy(dy.at[0], DY, in_sem.at[4])
    loop(4, lambda t: x_in(t).start())
    w_start(0)
    w_start(1)
    dy_in.start()

    def scale_of(w):
        return lax.rsqrt(jnp.mean(w * w, -1, keepdims=True) + 1e-6)

    def norm_x(t):
        x_in(t).wait()
        w = H[rows(t), :].astype(f32)
        A0[rows(t), :] = (w * scale_of(w)).astype(bf16)

    loop(4, norm_x)
    ACC[...] = jnp.zeros_like(ACC)

    def forward(i):
        w_wait(2 * i)
        w_wait(2 * i + 1)
        w_start(2 * i + 2)
        w_start(2 * i + 3)
        pair = lax.rem(i, SLOTS // 2)
        a = A0[...]
        g = dot(a, WGU[pair, :, 0 : 2 * FC])
        u = dot(a, WGU[pair, :, 2 * FC : 4 * FC])
        ACC[...] += dot((g * sigmoid(g) * u).astype(bf16), WD[pl.ds(2 * pair, 2)].reshape(2 * FC, d))
        t = rows(lax.rem(i, 4))
        DYT[:, t] = DY[t, :].T

    dy_in.wait()
    loop(chunks // 2, forward)

    def between(t):
        r = rows(t)
        h = (H[r, :].astype(f32) + ACC[r, :].astype(bf16).astype(f32)).astype(bf16)
        H[r, :] = h
        w = h.astype(f32)
        a = (w * scale_of(w)).astype(bf16)
        A1[r, :] = a
        AT[:, r] = a.T
        ACC[r, :] = jnp.zeros((step_rows, d), f32)

    loop(4, between)
    pl.semaphore_wait(bar, n - 1)

    def piece(s, h):
        return 2 * lax.rem(me + sign[h] * (1 + s) + 2 * n, n) + h

    def rs_copy(u, s, h):
        return pltpu.make_async_remote_copy(PART.at[u, piece(s, h)], RECV.at[u, s, h], rs_s.at[u], rs_r.at[u, s],
                                            device_id=(rep, to[h]), device_id_type=MESH)

    def whole(ref, sem):
        return pltpu.make_async_copy(ref, ref, sem)

    def rs_take(u, s, h):
        p = piece(s + 1, h)
        total = (PART[u, p].astype(f32) + RECV[u, s, h].astype(f32)).astype(bf16)
        PART[u, p] = total
        return total

    def rs_event(u, s):
        whole(RECV.at[u, s - 1], rs_r.at[u, s - 1]).wait()

        @pl.when(s < n - 1)
        def _():
            for h in (0, 1):
                rs_take(u, s - 1, h)
            for h in (0, 1):
                rs_copy(u, s, h).start()

        @pl.when(s == n - 1)
        def _():
            for h in (0, 1):
                g = rs_take(u, n - 2, h).astype(f32)
                SQ[...] += g * g
                own_copy(u, h).start()

    def own_copy(u, h):
        return pltpu.make_async_copy(PART.at[u, 2 * me + h], G.at[h, 0, u], own_sem.at[0])

    def events(i, back, number):
        def one(q):
            s = back - q

            @pl.when(i >= s)
            def _():
                rs_event(i - s, s)

        loop(number, one)

    def backward(ly, A, i):
        w_wait(i + chunks)

        @pl.when(i + 2 < units)
        def _():
            w_start(i + chunks + 2)

        slot = lax.rem(i + chunks, SLOTS)
        wgu = WGU.at[slot // 2, :, pl.ds(pl.multiple_of(lax.rem(slot, 2) * 2 * FC, 2 * FC), 2 * FC)]
        wd = WD.at[slot]

        def tile(t):
            r = pl.ds(pl.multiple_of(t * TILE, TILE), TILE)
            gu = dot(A[r, :], wgu[...])
            g, u = gu[:, :FC], gu[:, FC:]
            by_hid = dot_nt(DY[r, :], wd[...]).astype(bf16).astype(f32)
            sg = sigmoid(g)
            sl = g * sg
            HID[r, :] = (sl * u).astype(bf16)
            DGU[r, FC : 2 * FC] = (by_hid * sl).astype(bf16)
            DGU[r, 0:FC] = (by_hid * u * (sg + sl * (1 - sg))).astype(bf16)
            events(i, jnp.where(t == 0, n - 1, (n - 2) // 2), jnp.where(t == 0, n // 2, (n - 2) // 2 - 1))

        loop(tokens // TILE, tile)
        wdt = dot(DYT[...], HID[...]).astype(bf16).T
        for k in range(d // FC):
            PART[i, :, 2 * rows_p + k * rows_d : 2 * rows_p + (k + 1) * rows_d] = wdt[:, k * FC : (k + 1) * FC].reshape(2 * n, rows_d, FC)
        events(i, 1, 1)
        gw = dot(AT[...], DGU[...]).astype(bf16)
        PART[i, :, 0:rows_p] = gw[:, :FC].reshape(2 * n, rows_p, FC)
        PART[i, :, rows_p : 2 * rows_p] = gw[:, FC:].reshape(2 * n, rows_p, FC)

        for h in (0, 1):
            rs_copy(i, 0, h).start()
        if ly:
            ACC[...] += dot_nt(DGU[...], wgu[...])

    SQ[...] = jnp.zeros_like(SQ)
    loop(chunks, functools.partial(backward, 1, A1))

    def by_input(t):
        r = rows(t)
        w, da = H[r, :].astype(f32), ACC[r, :].astype(bf16).astype(f32)
        s = scale_of(w)
        along = jnp.sum(da * w, -1, keepdims=True) * (s * s * s) * (1.0 / d)
        by_h = (DY[r, :].astype(f32) + (da * s - w * along).astype(bf16).astype(f32)).astype(bf16)
        DY[r, :] = by_h
        DYT[:, r] = by_h.T
        AT[:, r] = A0[r, :].T

    loop(4, by_input)
    loop(chunks, lambda i: backward(0, A0, i + chunks))

    groups = units // JOINT

    def ag_copy(g, j, h, part=None):
        us = pl.ds(JOINT * g, JOINT)
        src = PART.at[us, 2 * me + h] if isinstance(j, int) and j == 0 else G.at[h, j, us]
        dst = G.at[h, j + 1, us] if part is None else last[part][h].at[pl.ds(JOINT * (g - part * groups // layers), JOINT)]
        return pltpu.make_async_remote_copy(src, dst, ag_s.at[g], ag_r.at[g, j], device_id=(rep, to[h]), device_id_type=MESH)

    def ag_wait(g, j):
        whole(RECV.at[0:JOINT, 0], ag_r.at[g, j]).wait()

    def drain(i):
        def one(q):
            u = units + i - n + 1 + q
            s = n - 1 - q

            @pl.when(u < units)
            def _():
                rs_event(u, s)

        loop(n - 1, one)

        def first(k):
            g = groups * i // (n - 1) + k

            @pl.when(g < groups * (i + 1) // (n - 1))
            def _():
                for h in (0, 1):
                    ag_copy(g, 0, h).start()

        loop(-(-groups // (n - 1)), first)

    loop(n - 1, drain)

    lanes = SQA.shape[-1]
    q = SQ[...]
    q = sum(q[:, k * lanes : (k + 1) * lanes] for k in range(FC // lanes))
    SQA[me] = q.reshape(-1, 8, lanes).sum(0)

    def sq_copy(k):
        return pltpu.make_async_remote_copy(SQA.at[me], SQA.at[me], sq_sem.at[0], sq_sem.at[1], device_id=(rep, lax.rem(me + k, n)), device_id_type=MESH)

    for k in range(1, n):
        sq_copy(k).start()

    def gather(t):
        j, g = t // groups, lax.rem(t, groups)
        ag_wait(g, j)
        for h in (0, 1):
            ag_copy(g, j + 1, h).start()

    loop((rounds - 2) * groups, gather)

    def gather_last(part, g):
        g = g + part * groups // layers
        ag_wait(g, rounds - 2)
        for h in (0, 1):
            ag_copy(g, rounds - 1, h, part).start()

    for part in range(layers):
        loop(groups // layers, functools.partial(gather_last, part))
    whole(SQA.at[1:n], sq_sem.at[1]).wait()
    total = SQA[0]
    for k in range(1, n):
        total = total + SQA[k]
    sq_out[...] = jnp.broadcast_to(jnp.sum(total, keepdims=True), sq_out.shape)

    def finish(u):
        whole(RECV.at[u], rs_s.at[u]).wait()

    def finish_ag(g):
        ag_wait(g, rounds - 1)
        whole(RECV.at[0:JOINT, 0:rounds], ag_s.at[g]).wait()

    loop(groups, finish_ag)
    loop(units, finish)
    whole(RECV.at[:, 0], own_sem.at[0]).wait()
    whole(SQA.at[1:n], sq_sem.at[0]).wait()


def train(n, rounds, x, dy, w_gate, w_up, w_down):
    _, tokens, d = x.shape
    layers, _, ff = w_gate.shape
    units, rows = layers * ff // FC, 3 * d // (2 * n)
    part = (rows, FC)
    any_ = pl.BlockSpec(memory_space=pl.ANY)
    got = jax.ShapeDtypeStruct((units // layers,) + part, bf16)
    act = pltpu.VMEM((tokens, d), bf16)
    act_t = pltpu.VMEM((d, tokens), bf16)
    dma = pltpu.SemaphoreType.DMA
    return pl.pallas_call(
        functools.partial(train_kernel, n, rounds),
        name="train",
        out_shape=(jax.ShapeDtypeStruct((2, rounds, units) + part, bf16), got, got, got, got, jax.ShapeDtypeStruct((8, 128), f32)),
        in_specs=[any_] * 5,
        out_specs=(any_,) * 5 + (pl.BlockSpec(memory_space=pltpu.VMEM),),
        scratch_shapes=[
            act, act, act_t, act, act, act_t,
            pltpu.VMEM((tokens, d), f32),
            pltpu.VMEM((tokens, FC), bf16),
            pltpu.VMEM((tokens, 2 * FC), bf16),
            pltpu.VMEM((SLOTS // 2, d, 4 * FC), bf16),
            pltpu.VMEM((SLOTS, FC, d), bf16),
            pltpu.VMEM((units, 2 * n) + part, bf16),
            pltpu.VMEM((units, n - 1, 2) + part, bf16),
            pltpu.VMEM(part, f32),
            pltpu.VMEM((n, 8, 128), f32),
            dma((5,)), dma((SLOTS, 3)),
            dma((units,)), dma((units, n - 1)), dma((units // JOINT,)), dma((units // JOINT, rounds)), dma((1,)), dma((2,)),
        ],
        compiler_params=pltpu.CompilerParams(collective_id=0, has_side_effects=True, vmem_limit_bytes=67043328),
        cost_estimate=pl.CostEstimate(flops=17 * 2 * tokens * d * ff, bytes_accessed=8 * units * n * rows * FC, transcendentals=0),
    )(x, dy, w_gate, w_up, w_down)


def adam_kernel(n, count, sources, spans, aliased, sq, *refs):
    n_src = len(spans)
    gs, w, m, v = refs[:n_src], refs[n_src : n_src + 3], refs[n_src + 3 : n_src + 6], refs[n_src + 6 : n_src + 9]
    refs = refs[n_src + 9 + (9 if aliased else 0) :]
    outs, g_in, wide, tall, in_sem, out_sem = refs[:9], refs[9], refs[10:13], refs[13:16], refs[16], refs[17]
    layers, _, rows_p, _ = w[0].shape
    _, chunks, _, rows_d, d = w[2].shape
    depth = g_in.shape[0]
    steps = len(sources)
    me = lax.axis_index("dp")
    h0, j0, b0 = sources[0]
    each = 1 if steps == 1 or sources[1][2] == b0 else layers

    def place(k):
        t = 2 * j0 + h0 + k // each
        h, j = lax.rem(t, 2), t // 2
        return b0 + lax.rem(k, each), 2 * lax.rem(me + (2 * h - 1) * j + n, n) + h

    def state(k, arrays, sem, out):
        back, p = place(k)
        ly = layers - 1 - back
        slot = lax.rem(k, depth)
        for q in range(3):
            for x in range(3):
                here = tall[q].at[slot] if x == 2 else wide[q].at[slot, x]
                there = arrays[3 * q + x].at[ly, :, p] if x == 2 else arrays[3 * q + x].at[ly, p]
                yield pltpu.make_async_copy(*((here, there) if out else (there, here)), sem.at[slot])

    def taken(k):
        return state(k, (*w, *m, *v), in_sem, False)

    def given(k):
        return state(k, outs, out_sem, True)

    def arrived(k, sem, times):
        slots = g_in.at[0:times]
        pltpu.make_async_copy(slots, slots, sem.at[lax.rem(k, depth)]).wait()

    def gradient(k, x):
        at = gs[x]
        if len(at.shape) == 5:
            t = 2 * j0 + h0 + k // each
            at = at.at[lax.rem(t, 2), t // 2, pl.ds(place(k)[0] * chunks, chunks)]
        slot = lax.rem(k, depth)
        return pltpu.make_async_copy(at, g_in.at[slot], in_sem.at[slot])

    def start(k):
        for c in taken(k):
            c.start()
        for x, (lo, hi) in enumerate(spans):

            @pl.when((k >= lo) & (k <= hi))
            def _():
                gradient(k, x).start()

    loop(min(depth - 2, steps), start)
    factor = jnp.minimum(1.0, 0.5 * lax.rsqrt(sq[0:1, 0:1] / count + 1e-30))

    def update(g, rows):
        g = g.astype(f32) * factor
        w, m, v = rows
        new_m = 0.9 * m[...] + 0.1 * g
        new_v = 0.95 * v[...] + 0.05 * g * g
        old = w[...].astype(f32)
        m[...] = new_m
        v[...] = new_v
        w[...] = (old - 0.02 * (new_m * lax.rsqrt(new_v + 1e-8) + 0.1 * old)).astype(bf16)

    def step(k):
        slot = lax.rem(k, depth)
        arrived(k, in_sem, 6)

        def chunk(c):
            cols = pl.ds(pl.multiple_of(c * FC, FC), FC)
            for x in range(2):
                update(g_in[slot, c, x * rows_p : (x + 1) * rows_p], [a.at[slot, x, :, cols] for a in wide])
            for x in range(d // FC):
                at = 2 * rows_p + x * rows_d
                update(g_in[slot, c, at : at + rows_d], [a.at[slot, c, :, x * FC : (x + 1) * FC] for a in tall])

        loop(chunks, chunk)
        for c in given(k):
            c.start()

        @pl.when(k >= 2)
        def _():
            arrived(k - 2, out_sem, 5)

        @pl.when(k + depth - 2 < steps)
        def _():
            start(k + depth - 2)

    loop(steps, step)

    def finish(k):
        arrived(steps - 2 + k, out_sem, 5)

    loop(2, finish)


def adam(views, prev, sq, steps, n, count):
    gs, spans = [], []
    for k, (g, *_) in enumerate(steps):
        if gs and gs[-1] is g:
            spans[-1][1] = k
        else:
            gs.append(g)
            spans.append([k, k])
    sources = [src[1:] for src in steps]
    w, m, v = views
    layers, parts, rows_p, ff = w[0].shape
    _, chunks, _, rows_d, d = w[2].shape
    any_ = pl.BlockSpec(memory_space=pl.ANY)
    args = [*gs, *w, *m, *v]
    aliases = {}
    if prev is not None:
        aliases = {1 + len(args) + k: k for k in range(9)}
        args += list(prev)
    moved = 2 * len(sources) * sum(a.size * a.dtype.itemsize for a in (*w, *m, *v)) // (parts * layers)
    types = (bf16, f32, f32)
    return pl.pallas_call(
        functools.partial(adam_kernel, n, count, sources, spans, prev is not None),
        name="adam",
        in_specs=[pl.BlockSpec(memory_space=pltpu.VMEM)] + [any_] * len(args),
        out_specs=[any_] * 9,
        out_shape=[jax.ShapeDtypeStruct(a.shape, a.dtype) for a in (*w, *m, *v)],
        input_output_aliases=aliases,
        scratch_shapes=[pltpu.VMEM((DEPTH, chunks, gs[0].shape[-2], FC), bf16)]
        + [pltpu.VMEM((DEPTH, 2, rows_p, ff), t) for t in types]
        + [pltpu.VMEM((DEPTH, chunks, rows_d, d), t) for t in types]
        + [pltpu.SemaphoreType.DMA((DEPTH,)), pltpu.SemaphoreType.DMA((DEPTH,))],
        compiler_params=pltpu.CompilerParams(vmem_limit_bytes=67043328),
        cost_estimate=pl.CostEstimate(flops=30 * moved, bytes_accessed=moved, transcendentals=0),
    )(sq, *args)


def solution(mesh):
    n = mesh.shape["dp"]

    def step(x, dy, *arrays):
        w = arrays[0:3]
        count = 3 * w[0].size
        rounds = HELD
        return whole(n, rounds, count, x, dy, arrays)

    def whole(n, rounds, count, x, dy, arrays):
        w = arrays[0:3]
        layers, d, ff = w[0].shape
        G, *got, sq = train(n, rounds, x, dy, *w)

        def view(a):
            a = list(a)
            for k in range(2):
                a[k] = a[k].reshape(layers, 2 * n, d // (2 * n), ff)
            a[2] = a[2].reshape(layers, ff // FC, 2 * n, FC // (2 * n), d)
            return a

        views = tuple(view(arrays[k : k + 3]) for k in (0, 3, 6))
        right, left = [(k, (k + 1) % n) for k in range(n)], [(k, (k - 1) % n) for k in range(n)]

        out, hops = None, n - 1 - rounds
        came, at = [[got[2 * b : 2 * b + 2] for b in range(layers)]], 0

        def steps_of(p, b):
            j, h = p // 2, p % 2
            return G if j < rounds else came[j - rounds][b][h], h, j, b

        for k in range(hops):
            came.append([])
            for b in range(layers):
                pair = []
                for h, way in enumerate((right, left)):
                    pair.append(lax.ppermute(came[k][b][h], "dp", way))
                came[-1].append(pair)
            more = -(-(2 * n - 2 - at) // (hops - k))
            out = adam(views, out, sq, [steps_of(p, b) for p in range(at, at + more) for b in range(layers)], n, count)
            at += more
        for b in range(layers):
            out = adam(views, out, sq, [steps_of(p, b) for p in range(at, 2 * n)], n, count)
        return tuple(o.reshape(a.shape) for o, a in zip(out, arrays, strict=True))

    return jax.shard_map(
        step,
        mesh=mesh,
        in_specs=(P(("rep", "dp"), None, None),) * 2 + (P(None, None, None),) * 9,
        out_specs=(P("rep", None, None),) * 9,
        check_vma=False,
    )
```

```python
import functools

import jax
import jax.numpy as jnp
from jax import lax
from jax.experimental import pallas as pl
from jax.experimental.pallas import tpu as pltpu
from jax.sharding import PartitionSpec as P


f32, bf16 = jnp.float32, jnp.bfloat16
MESH = pl.DeviceIdType.MESH
FC = 256
SLOTS = 4
JOINT = 2
HELD = 3
DEPTH = 6
TILE = 1024


def dot(a, b):
    return jnp.dot(a, b, preferred_element_type=f32)


def dot_nt(a, b):
    return lax.dot_general(a, b, (((1,), (1,)), ((), ())), preferred_element_type=f32)


def sigmoid(x):
    return 0.5 * jnp.tanh(0.5 * x) + 0.5


def loop(n, body):
    lax.fori_loop(0, n, lambda i, c: (body(i), c)[1], 0)


def train_kernel(n, rounds, x, dy, wg_h, wu_h, wd_h, G, L0, L1, sq_out, A0, A1, AT, H, DY, DYT, ACC, HID, DGU, WGU, WD, PART, RECV, SQ, SQA, SQO,
                 in_sem, w_sem, rs_s, rs_r, ag_s, ag_r, own_sem, sq_sem):
    _, tokens, d = x.shape
    layers, _, ff = wg_h.shape
    chunks = ff // FC
    units = layers * chunks
    last = (L0, L1)
    rows_p, rows_d = d // (2 * n), FC // (2 * n)
    me, rep = lax.axis_index("dp"), lax.axis_index("rep")
    to = (lax.rem(me + 1, n), lax.rem(me + n - 1, n))
    sign = (-1, 1)
    step_rows = tokens // 4

    bar = pltpu.get_barrier_semaphore()
    for k in range(1, n):
        pl.semaphore_signal(bar, inc=1, device_id=(rep, lax.rem(me + k, n)), device_id_type=MESH)

    def w_copies(i):
        slot = lax.rem(i, SLOTS)
        ly = jnp.where(i // chunks == 1, layers - 1, 0)
        c = pl.ds(pl.multiple_of(lax.rem(i, chunks) * FC, FC), FC)
        half = lax.rem(slot, 2)
        first = i < chunks
        at = jnp.where(first, half, 2 * half) * FC
        gap = jnp.where(first, 2, 1) * FC
        return (
            pltpu.make_async_copy(wg_h.at[ly, :, c], WGU.at[slot // 2, :, pl.ds(pl.multiple_of(at, FC), FC)], w_sem.at[slot, 0]),
            pltpu.make_async_copy(wu_h.at[ly, :, c], WGU.at[slot // 2, :, pl.ds(pl.multiple_of(at + gap, FC), FC)], w_sem.at[slot, 1]),
            pltpu.make_async_copy(wd_h.at[ly, c, :], WD.at[slot], w_sem.at[slot, 2]),
        )

    def w_start(i):
        for c in w_copies(i):
            c.start()

    def w_wait(i):
        for c in w_copies(i):
            c.wait()

    def rows(t):
        return pl.ds(pl.multiple_of(t * step_rows, step_rows), step_rows)

    def x_in(t):
        return pltpu.make_async_copy(x.at[0, rows(t)], H.at[rows(t)], in_sem.at[t])

    dy_in = pltpu.make_async_copy(dy.at[0], DY, in_sem.at[4])
    loop(4, lambda t: x_in(t).start())
    w_start(0)
    w_start(1)
    dy_in.start()

    def scale_of(w):
        return lax.rsqrt(jnp.mean(w * w, -1, keepdims=True) + 1e-6)

    def norm_x(t):
        x_in(t).wait()
        w = H[rows(t), :].astype(f32)
        A0[rows(t), :] = (w * scale_of(w)).astype(bf16)

    loop(4, norm_x)
    ACC[...] = jnp.zeros_like(ACC)

    def forward(i):
        w_wait(2 * i)
        w_wait(2 * i + 1)
        w_start(2 * i + 2)
        w_start(2 * i + 3)
        pair = lax.rem(i, SLOTS // 2)
        a = A0[...]
        g = dot(a, WGU[pair, :, 0 : 2 * FC])
        u = dot(a, WGU[pair, :, 2 * FC : 4 * FC])
        ACC[...] += dot((g * sigmoid(g) * u).astype(bf16), WD[pl.ds(2 * pair, 2)].reshape(2 * FC, d))
        t = rows(lax.rem(i, 4))
        DYT[:, t] = DY[t, :].T

    dy_in.wait()
    loop(chunks // 2, forward)

    def between(t):
        r = rows(t)
        h = (H[r, :].astype(f32) + ACC[r, :].astype(bf16).astype(f32)).astype(bf16)
        H[r, :] = h
        w = h.astype(f32)
        a = (w * scale_of(w)).astype(bf16)
        A1[r, :] = a
        AT[:, r] = a.T
        ACC[r, :] = jnp.zeros((step_rows, d), f32)

    loop(4, between)
    pl.semaphore_wait(bar, n - 1)

    def piece(s, h):
        return 2 * lax.rem(me + sign[h] * (1 + s) + 2 * n, n) + h

    def rs_copy(u, s, h):
        return pltpu.make_async_remote_copy(PART.at[u, piece(s, h)], RECV.at[u, s, h], rs_s.at[u], rs_r.at[u, s],
                                            device_id=(rep, to[h]), device_id_type=MESH)

    def whole(ref, sem):
        return pltpu.make_async_copy(ref, ref, sem)

    def rs_take(u, s, h):
        p = piece(s + 1, h)
        total = (PART[u, p].astype(f32) + RECV[u, s, h].astype(f32)).astype(bf16)
        PART[u, p] = total
        return total

    def rs_event(u, s):
        whole(RECV.at[u, s - 1], rs_r.at[u, s - 1]).wait()

        @pl.when(s < n - 1)
        def _():
            for h in (0, 1):
                rs_take(u, s - 1, h)
            for h in (0, 1):
                rs_copy(u, s, h).start()

        @pl.when(s == n - 1)
        def _():
            for h in (0, 1):
                g = rs_take(u, n - 2, h).astype(f32)
                SQ[...] += g * g
                own_copy(u, h).start()

    def own_copy(u, h):
        return pltpu.make_async_copy(PART.at[u, 2 * me + h], G.at[h, 0, u], own_sem.at[0])

    def events(i, back, number):
        def one(q):
            s = back - q

            @pl.when(i >= s)
            def _():
                rs_event(i - s, s)

        loop(number, one)

    def backward(ly, A, i):
        w_wait(i + chunks)

        @pl.when(i + 2 < units)
        def _():
            w_start(i + chunks + 2)

        slot = lax.rem(i + chunks, SLOTS)
        wgu = WGU.at[slot // 2, :, pl.ds(pl.multiple_of(lax.rem(slot, 2) * 2 * FC, 2 * FC), 2 * FC)]
        wd = WD.at[slot]

        def tile(t):
            r = pl.ds(pl.multiple_of(t * TILE, TILE), TILE)
            gu = dot(A[r, :], wgu[...])
            g, u = gu[:, :FC], gu[:, FC:]
            by_hid = dot_nt(DY[r, :], wd[...]).astype(bf16).astype(f32)
            sg = sigmoid(g)
            sl = g * sg
            HID[r, :] = (sl * u).astype(bf16)
            DGU[r, FC : 2 * FC] = (by_hid * sl).astype(bf16)
            DGU[r, 0:FC] = (by_hid * u * (sg + sl * (1 - sg))).astype(bf16)
            events(i, jnp.where(t == 0, n - 1, (n - 2) // 2), jnp.where(t == 0, n // 2, (n - 2) // 2 - 1))

        loop(tokens // TILE, tile)
        wdt = dot(DYT[...], HID[...]).astype(bf16).T
        for k in range(d // FC):
            PART[i, :, 2 * rows_p + k * rows_d : 2 * rows_p + (k + 1) * rows_d] = wdt[:, k * FC : (k + 1) * FC].reshape(2 * n, rows_d, FC)
        events(i, 1, 1)
        gw = dot(AT[...], DGU[...]).astype(bf16)
        PART[i, :, 0:rows_p] = gw[:, :FC].reshape(2 * n, rows_p, FC)
        PART[i, :, rows_p : 2 * rows_p] = gw[:, FC:].reshape(2 * n, rows_p, FC)

        for h in (0, 1):
            rs_copy(i, 0, h).start()
        if ly:
            ACC[...] += dot_nt(DGU[...], wgu[...])

    SQ[...] = jnp.zeros_like(SQ)
    loop(chunks, functools.partial(backward, 1, A1))

    def by_input(t):
        r = rows(t)
        w, da = H[r, :].astype(f32), ACC[r, :].astype(bf16).astype(f32)
        s = scale_of(w)
        along = jnp.sum(da * w, -1, keepdims=True) * (s * s * s) * (1.0 / d)
        by_h = (DY[r, :].astype(f32) + (da * s - w * along).astype(bf16).astype(f32)).astype(bf16)
        DY[r, :] = by_h
        DYT[:, r] = by_h.T
        AT[:, r] = A0[r, :].T

    loop(4, by_input)
    loop(chunks, lambda i: backward(0, A0, i + chunks))

    groups = units // JOINT

    def ag_copy(g, j, h):
        us = pl.ds(JOINT * g, JOINT)
        src = PART.at[us, 2 * me + h] if isinstance(j, int) and j == 0 else G.at[h, j, us]
        dst = last[h].at[us] if isinstance(j, int) and j == rounds - 1 else G.at[h, j + 1, us]
        return pltpu.make_async_remote_copy(src, dst, ag_s.at[g], ag_r.at[g, j], device_id=(rep, to[h]), device_id_type=MESH)

    def ag_wait(g, j):
        whole(RECV.at[0:JOINT, 0], ag_r.at[g, j]).wait()

    def drain(i):
        def one(q):
            u = units + i - n + 1 + q
            s = n - 1 - q

            @pl.when(u < units)
            def _():
                rs_event(u, s)

        loop(n - 1, one)

        def first(k):
            g = groups * i // (n - 1) + k

            @pl.when(g < groups * (i + 1) // (n - 1))
            def _():
                for h in (0, 1):
                    ag_copy(g, 0, h).start()

        loop(-(-groups // (n - 1)), first)

    loop(n - 1, drain)

    lanes = SQA.shape[-1]
    q = SQ[...]
    q = sum(q[:, k * lanes : (k + 1) * lanes] for k in range(FC // lanes))
    SQA[me] = q.reshape(-1, 8, lanes).sum(0)

    def sq_copy(k):
        return pltpu.make_async_remote_copy(SQA.at[me], SQA.at[me], sq_sem.at[0], sq_sem.at[1], device_id=(rep, lax.rem(me + k, n)), device_id_type=MESH)

    for k in range(1, n):
        sq_copy(k).start()

    def gather(t):
        j, g = t // groups, lax.rem(t, groups)
        ag_wait(g, j)
        for h in (0, 1):
            ag_copy(g, j + 1, h).start()

    loop((rounds - 2) * groups, gather)

    def gather_last(g):
        ag_wait(g, rounds - 2)
        for h in (0, 1):
            ag_copy(g, rounds - 1, h).start()

    loop(groups, gather_last)
    whole(SQA.at[1:n], sq_sem.at[1]).wait()
    total = SQA[0]
    for k in range(1, n):
        total = total + SQA[k]
    SQO[...] = jnp.broadcast_to(jnp.sum(total, keepdims=True), SQO.shape)
    sq_copy_out = pltpu.make_async_copy(SQO, sq_out, own_sem.at[1])

    def finish(u):
        whole(RECV.at[u], rs_s.at[u]).wait()

    def finish_ag(g):
        ag_wait(g, rounds - 1)
        whole(RECV.at[0:JOINT, 0:rounds], ag_s.at[g]).wait()

    loop(units, finish)
    sq_copy_out.start()
    loop(groups, finish_ag)
    sq_copy_out.wait()
    whole(RECV.at[:, 0], own_sem.at[0]).wait()
    whole(SQA.at[1:n], sq_sem.at[0]).wait()


def train(n, rounds, x, dy, w_gate, w_up, w_down):
    _, tokens, d = x.shape
    layers, _, ff = w_gate.shape
    units, rows = layers * ff // FC, 3 * d // (2 * n)
    part = (rows, FC)
    any_ = pl.BlockSpec(memory_space=pl.ANY)
    got = jax.ShapeDtypeStruct((units,) + part, bf16)
    act = pltpu.VMEM((tokens, d), bf16)
    act_t = pltpu.VMEM((d, tokens), bf16)
    dma = pltpu.SemaphoreType.DMA
    return pl.pallas_call(
        functools.partial(train_kernel, n, rounds),
        name="train",
        out_shape=(jax.ShapeDtypeStruct((2, rounds, units) + part, bf16), got, got, jax.ShapeDtypeStruct((8, 128), f32)),
        in_specs=[any_] * 5,
        out_specs=(any_,) * 4,
        scratch_shapes=[
            act, act, act_t, act, act, act_t,
            pltpu.VMEM((tokens, d), f32),
            pltpu.VMEM((tokens, FC), bf16),
            pltpu.VMEM((tokens, 2 * FC), bf16),
            pltpu.VMEM((SLOTS // 2, d, 4 * FC), bf16),
            pltpu.VMEM((SLOTS, FC, d), bf16),
            pltpu.VMEM((units, 2 * n) + part, bf16),
            pltpu.VMEM((units, n - 1, 2) + part, bf16),
            pltpu.VMEM(part, f32),
            pltpu.VMEM((n, 8, 128), f32),
            pltpu.VMEM((8, 128), f32),
            dma((5,)), dma((SLOTS, 3)),
            dma((units,)), dma((units, n - 1)), dma((units // JOINT,)), dma((units // JOINT, rounds)), dma((2,)), dma((2,)),
        ],
        compiler_params=pltpu.CompilerParams(collective_id=0, has_side_effects=True, vmem_limit_bytes=67043328),
        cost_estimate=pl.CostEstimate(flops=17 * 2 * tokens * d * ff, bytes_accessed=8 * units * n * rows * FC, transcendentals=0),
    )(x, dy, w_gate, w_up, w_down)


def place_of(k, me, n, layers, first):
    t = first + k // layers
    h, j = lax.rem(t, 2), t // 2
    return lax.rem(k, layers), 2 * lax.rem(me + (2 * h - 1) * j + n, n) + h


def stage_kernel(n, first, *refs):
    arrays, wide, tall, sem = refs[:9], refs[9:12], refs[12:15], refs[15]
    layers, steps = arrays[0].shape[0], wide[0].shape[0]
    me = lax.axis_index("dp")

    def copies(k):
        ly, p = place_of(k, me, n, layers, first)
        for q in range(3):
            for x in range(3):
                here = tall[q].at[k] if x == 2 else wide[q].at[k, x]
                there = arrays[3 * q + x].at[ly, :, p] if x == 2 else arrays[3 * q + x].at[ly, p]
                yield pltpu.make_async_copy(there, here, sem.at[q, x])

    def start(k):
        for c in copies(k):
            c.start()

    loop(steps, start)
    for q in range(3):
        for x in range(2):
            both = wide[q].at[:, x]
            pltpu.make_async_copy(both, both, sem.at[q, x]).wait()
        pltpu.make_async_copy(tall[q], tall[q], sem.at[q, 2]).wait()


def stage(views, first, steps, n):
    w, m, v = views
    _, _, rows_p, ff = w[0].shape
    _, chunks, _, rows_d, d = w[2].shape
    types = (bf16, f32, f32)
    shapes = [jax.ShapeDtypeStruct((steps, 2, rows_p, ff), t) for t in types] + [jax.ShapeDtypeStruct((steps, chunks, rows_d, d), t) for t in types]
    return pl.pallas_call(
        functools.partial(stage_kernel, n, first),
        name="stage",
        in_specs=[pl.BlockSpec(memory_space=pltpu.HBM)] * 9,
        out_specs=[pl.BlockSpec(memory_space=pltpu.VMEM)] * 6,
        out_shape=shapes,
        scratch_shapes=[pltpu.SemaphoreType.DMA((3, 3))],
        compiler_params=pltpu.CompilerParams(vmem_limit_bytes=44 << 20),
        cost_estimate=pl.CostEstimate(flops=3000000000, bytes_accessed=10000000, transcendentals=0),
    )(*w, *m, *v)


def adam_kernel(n, count, sources, n_src, aliased, staged, sq, *refs):
    gs, w, m, v = refs[:n_src], refs[n_src : n_src + 3], refs[n_src + 3 : n_src + 6], refs[n_src + 6 : n_src + 9]
    if staged:
        old_wide, old_tall = refs[n_src : n_src + 3], refs[n_src + 3 : n_src + 6]
        refs = refs[n_src + 6 + (9 if aliased else 0) :]
        w = refs[:3]
    else:
        refs = refs[n_src + 9 + (9 if aliased else 0) :]
    outs, g_in, wide, tall, in_sem, out_sem = refs[:9], refs[9], refs[10:13], refs[13:16], refs[16], refs[17]
    layers, _, rows_p, _ = w[0].shape
    _, chunks, _, rows_d, d = w[2].shape
    depth = g_in.shape[0]
    steps = layers * len(sources)
    me = lax.axis_index("dp")
    _, h0, j0 = sources[0]

    def place(k):
        return place_of(k, me, n, layers, 2 * j0 + h0)

    def state(k, arrays, sem, out):
        ly, p = place(k)
        slot = lax.rem(k, depth)
        for q in range(3):
            for x in range(3):
                here = tall[q].at[slot] if x == 2 else wide[q].at[slot, x]
                there = arrays[3 * q + x].at[ly, :, p] if x == 2 else arrays[3 * q + x].at[ly, p]
                yield pltpu.make_async_copy(*((here, there) if out else (there, here)), sem.at[slot])

    def taken(k):
        return state(k, (*w, *m, *v), in_sem, False)

    def given(k):
        return state(k, outs, out_sem, True)

    def arrived(k, sem, times):
        slots = g_in.at[0:times]
        pltpu.make_async_copy(slots, slots, sem.at[lax.rem(k, depth)]).wait()

    def gradient(k, x, t):
        units = pl.ds((layers - 1 - lax.rem(k, layers)) * chunks, chunks)
        at = gs[x].at[units]
        if len(gs[x].shape) == 5:
            i = 2 * sources[t][2] + sources[t][1] + k // layers - t
            at = gs[x].at[lax.rem(i, 2), i // 2, units]
        slot = lax.rem(k, depth)
        return pltpu.make_async_copy(at, g_in.at[slot], in_sem.at[slot])

    spans = [[t for t, src in enumerate(sources) if src[0] == x] for x in range(n_src)]

    def start(k):
        if not staged:
            for c in taken(k):
                c.start()
        for x, span in enumerate(spans):

            @pl.when((k >= layers * span[0]) & (k < layers * (span[-1] + 1)))
            def _():
                gradient(k, x, span[0]).start()

    loop(min(depth - 2, steps), start)
    factor = jnp.minimum(1.0, 0.5 * lax.rsqrt(sq[0:1, 0:1] / count + 1e-30))

    def update(g, arrays, old_arrays, at):
        g = g.astype(f32) * factor
        w, m, v = (a.at[at] for a in arrays)
        old_w, old_m, old_v = (a.at[at] for a in old_arrays)
        new_m = 0.9 * old_m[...] + 0.1 * g
        new_v = 0.95 * old_v[...] + 0.05 * g * g
        old = old_w[...].astype(f32)
        m[...] = new_m
        v[...] = new_v
        w[...] = (old - 0.02 * (new_m * lax.rsqrt(new_v + 1e-8) + 0.1 * old)).astype(bf16)

    def step(k):
        slot = lax.rem(k, depth)
        arrived(k, in_sem, 1 if staged else 6)

        def chunk(c):
            cols = pl.ds(pl.multiple_of(c * FC, FC), FC)
            for x in range(2):
                update(g_in[slot, c, x * rows_p : (x + 1) * rows_p], wide, old_wide if staged else wide, (slot, x, slice(None), cols))
            for x in range(d // FC):
                at = 2 * rows_p + x * rows_d
                update(g_in[slot, c, at : at + rows_d], tall, old_tall if staged else tall, (slot, c, slice(None), slice(x * FC, (x + 1) * FC)))

        loop(chunks, chunk)
        for c in given(k):
            c.start()

        @pl.when(k >= 2)
        def _():
            arrived(k - 2, out_sem, 5)

        @pl.when(k + depth - 2 < steps)
        def _():
            start(k + depth - 2)

    loop(steps, step)

    def finish(k):
        arrived(steps - 2 + k, out_sem, 5)

    loop(2, finish)


def adam(views, prev, sq, gs, sources, n, count, staged=None):
    w, m, v = views
    _, parts, rows_p, ff = w[0].shape
    _, chunks, _, rows_d, d = w[2].shape
    any_, vmem = pl.BlockSpec(memory_space=pl.ANY), pl.BlockSpec(memory_space=pltpu.VMEM)
    args = [*gs, *(staged or (*w, *m, *v))]
    aliases = {}
    if prev is not None:
        aliases = {1 + len(args) + k: k for k in range(9)}
        args += list(prev)
    moved = 2 * len(sources) * sum(a.size * a.dtype.itemsize for a in (*w, *m, *v)) // parts
    types = (bf16, f32, f32)
    return pl.pallas_call(
        functools.partial(adam_kernel, n, count, sources, len(gs), prev is not None, bool(staged)),
        name="adam",
        in_specs=[vmem] + [any_] * len(gs) + [vmem if staged else any_] * (6 if staged else 9) + [any_] * (0 if prev is None else 9),
        out_specs=[any_] * 9,
        out_shape=[jax.ShapeDtypeStruct(a.shape, a.dtype) for a in (*w, *m, *v)],
        input_output_aliases=aliases,
        scratch_shapes=[pltpu.VMEM((DEPTH, chunks, gs[0].shape[-2], FC), bf16)]
        + [pltpu.VMEM((DEPTH, 2, rows_p, ff), t) for t in types]
        + [pltpu.VMEM((DEPTH, chunks, rows_d, d), t) for t in types]
        + [pltpu.SemaphoreType.DMA((DEPTH,)), pltpu.SemaphoreType.DMA((DEPTH,))],
        compiler_params=pltpu.CompilerParams(vmem_limit_bytes=(44 << 20) if staged else 67043328),
        cost_estimate=pl.CostEstimate(flops=30 * moved, bytes_accessed=moved, transcendentals=0),
    )(sq, *args)


def solution(mesh):
    n = mesh.shape["dp"]

    def step(x, dy, *arrays):
        w = arrays[0:3]
        count = 3 * w[0].size
        rounds = HELD
        return whole(n, rounds, count, x, dy, arrays)

    def whole(n, rounds, count, x, dy, arrays):
        w = arrays[0:3]
        layers, d, ff = w[0].shape
        G, *got, sq = train(n, rounds, x, dy, *w)

        def view(a):
            a = list(a)
            for k in range(2):
                a[k] = a[k].reshape(layers, 2 * n, d // (2 * n), ff)
            a[2] = a[2].reshape(layers, ff // FC, 2 * n, FC // (2 * n), d)
            return a

        views = tuple(view(arrays[k : k + 3]) for k in (0, 3, 6))
        right, left = [(k, (k + 1) % n) for k in range(n)], [(k, (k - 1) % n) for k in range(n)]

        out, hops = None, n - 1 - rounds
        came, at = [got], 0
        for k in range(hops + 1):
            if k < hops:
                r = lax.ppermute(came[k][0], "dp", right)
                came.append([r, lax.ppermute(came[k][1], "dp", left)])
            gs, sources = [], []
            for p in range(at, at + (-(-(2 * n - 2 - at) // (hops - k)) if k < hops else 2)):
                j, h = p // 2, p % 2
                g = G if j < rounds else came[j - rounds][h]
                if not any(g is o for o in gs):
                    gs.append(g)
                sources.append((len(gs) - 1, h, j))
            at += len(sources)
            out = adam(views, out, sq, gs, sources, n, count, staged if k == hops else None)
            if k == hops - 1:
                staged = stage(views, at, 2 * layers, n)
        return tuple(o.reshape(a.shape) for o, a in zip(out, arrays, strict=True))

    return jax.shard_map(
        step,
        mesh=mesh,
        in_specs=(P(("rep", "dp"), None, None),) * 2 + (P(None, None, None),) * 9,
        out_specs=(P("rep", None, None),) * 9,
        check_vma=False,
    )
```

```python
import functools

import jax
import jax.numpy as jnp
from jax import lax
from jax.experimental import pallas as pl
from jax.experimental.pallas import tpu as pltpu
from jax.sharding import PartitionSpec as P


f32, bf16 = jnp.float32, jnp.bfloat16
MESH = pl.DeviceIdType.MESH
FC = 256
SLOTS = 4
JOINT = 2
HELD = 3
LIMITS = {1: 61 << 20, 0: 24 << 20}
DEPTH = 6
TILE = 1024


def dot(a, b):
    return jnp.dot(a, b, preferred_element_type=f32)


def dot_nt(a, b):
    return lax.dot_general(a, b, (((1,), (1,)), ((), ())), preferred_element_type=f32)


def sigmoid(x):
    return 0.5 * jnp.tanh(0.5 * x) + 0.5


def loop(n, body):
    lax.fori_loop(0, n, lambda i, c: (body(i), c)[1], 0)


def train_kernel(n, rounds, x, dy, wg_h, wu_h, wd_h, G, L0, L1, sq_out, A0, A1, AT, H, DY, DYT, ACC, HID, DGU, WGU, WD, PART, RECV, SQ, SQA, SQO,
                 in_sem, w_sem, rs_s, rs_r, ag_s, ag_r, own_sem, sq_sem):
    _, tokens, d = x.shape
    layers, _, ff = wg_h.shape
    chunks = ff // FC
    units = layers * chunks
    last = (L0, L1)
    rows_p, rows_d = d // (2 * n), FC // (2 * n)
    me, rep = lax.axis_index("dp"), lax.axis_index("rep")
    to = (lax.rem(me + 1, n), lax.rem(me + n - 1, n))
    sign = (-1, 1)
    step_rows = tokens // 4

    bar = pltpu.get_barrier_semaphore()
    for k in range(1, n):
        pl.semaphore_signal(bar, inc=1, device_id=(rep, lax.rem(me + k, n)), device_id_type=MESH)

    def w_copies(i):
        slot = lax.rem(i, SLOTS)
        ly = jnp.where(i // chunks == 1, layers - 1, 0)
        c = pl.ds(pl.multiple_of(lax.rem(i, chunks) * FC, FC), FC)
        half = lax.rem(slot, 2)
        first = i < chunks
        at = jnp.where(first, half, 2 * half) * FC
        gap = jnp.where(first, 2, 1) * FC
        return (
            pltpu.make_async_copy(wg_h.at[ly, :, c], WGU.at[slot // 2, :, pl.ds(pl.multiple_of(at, FC), FC)], w_sem.at[slot, 0]),
            pltpu.make_async_copy(wu_h.at[ly, :, c], WGU.at[slot // 2, :, pl.ds(pl.multiple_of(at + gap, FC), FC)], w_sem.at[slot, 1]),
            pltpu.make_async_copy(wd_h.at[ly, c, :], WD.at[slot], w_sem.at[slot, 2]),
        )

    def w_start(i):
        for c in w_copies(i):
            c.start()

    def w_wait(i):
        for c in w_copies(i):
            c.wait()

    def rows(t):
        return pl.ds(pl.multiple_of(t * step_rows, step_rows), step_rows)

    def x_in(t):
        return pltpu.make_async_copy(x.at[0, rows(t)], H.at[rows(t)], in_sem.at[t])

    dy_in = pltpu.make_async_copy(dy.at[0], DY, in_sem.at[4])
    loop(4, lambda t: x_in(t).start())
    w_start(0)
    w_start(1)
    dy_in.start()

    def scale_of(w):
        return lax.rsqrt(jnp.mean(w * w, -1, keepdims=True) + 1e-6)

    def norm_x(t):
        x_in(t).wait()
        w = H[rows(t), :].astype(f32)
        A0[rows(t), :] = (w * scale_of(w)).astype(bf16)

    loop(4, norm_x)
    ACC[...] = jnp.zeros_like(ACC)

    def forward(i):
        w_wait(2 * i)
        w_wait(2 * i + 1)
        w_start(2 * i + 2)
        w_start(2 * i + 3)
        pair = lax.rem(i, SLOTS // 2)
        a = A0[...]
        g = dot(a, WGU[pair, :, 0 : 2 * FC])
        u = dot(a, WGU[pair, :, 2 * FC : 4 * FC])
        ACC[...] += dot((g * sigmoid(g) * u).astype(bf16), WD[pl.ds(2 * pair, 2)].reshape(2 * FC, d))
        t = rows(lax.rem(i, 4))
        DYT[:, t] = DY[t, :].T

    dy_in.wait()
    loop(chunks // 2, forward)

    def between(t):
        r = rows(t)
        h = (H[r, :].astype(f32) + ACC[r, :].astype(bf16).astype(f32)).astype(bf16)
        H[r, :] = h
        w = h.astype(f32)
        a = (w * scale_of(w)).astype(bf16)
        A1[r, :] = a
        AT[:, r] = a.T
        ACC[r, :] = jnp.zeros((step_rows, d), f32)

    loop(4, between)
    pl.semaphore_wait(bar, n - 1)

    def piece(s, h):
        return 2 * lax.rem(me + sign[h] * (1 + s) + 2 * n, n) + h

    def rs_copy(u, s, h):
        return pltpu.make_async_remote_copy(PART.at[u, piece(s, h)], RECV.at[u, s, h], rs_s.at[u], rs_r.at[u, s],
                                            device_id=(rep, to[h]), device_id_type=MESH)

    def whole(ref, sem):
        return pltpu.make_async_copy(ref, ref, sem)

    def rs_take(u, s, h):
        p = piece(s + 1, h)
        total = (PART[u, p].astype(f32) + RECV[u, s, h].astype(f32)).astype(bf16)
        PART[u, p] = total
        return total

    def rs_event(u, s):
        whole(RECV.at[u, s - 1], rs_r.at[u, s - 1]).wait()

        @pl.when(s < n - 1)
        def _():
            for h in (0, 1):
                rs_take(u, s - 1, h)
            for h in (0, 1):
                rs_copy(u, s, h).start()

        @pl.when(s == n - 1)
        def _():
            for h in (0, 1):
                g = rs_take(u, n - 2, h).astype(f32)
                SQ[...] += g * g
                own_copy(u, h).start()

    def own_copy(u, h):
        return pltpu.make_async_copy(PART.at[u, 2 * me + h], G.at[h, 0, u], own_sem.at[0])

    def events(i, back, number):
        def one(q):
            s = back - q

            @pl.when(i >= s)
            def _():
                rs_event(i - s, s)

        loop(number, one)

    def backward(ly, A, i):
        w_wait(i + chunks)

        @pl.when(i + 2 < units)
        def _():
            w_start(i + chunks + 2)

        slot = lax.rem(i + chunks, SLOTS)
        wgu = WGU.at[slot // 2, :, pl.ds(pl.multiple_of(lax.rem(slot, 2) * 2 * FC, 2 * FC), 2 * FC)]
        wd = WD.at[slot]

        def tile(t):
            r = pl.ds(pl.multiple_of(t * TILE, TILE), TILE)
            gu = dot(A[r, :], wgu[...])
            g, u = gu[:, :FC], gu[:, FC:]
            by_hid = dot_nt(DY[r, :], wd[...]).astype(bf16).astype(f32)
            sg = sigmoid(g)
            sl = g * sg
            HID[r, :] = (sl * u).astype(bf16)
            DGU[r, FC : 2 * FC] = (by_hid * sl).astype(bf16)
            DGU[r, 0:FC] = (by_hid * u * (sg + sl * (1 - sg))).astype(bf16)
            events(i, jnp.where(t == 0, n - 1, (n - 2) // 2), jnp.where(t == 0, n // 2, (n - 2) // 2 - 1))

        loop(tokens // TILE, tile)
        wdt = dot(DYT[...], HID[...]).astype(bf16).T
        for k in range(d // FC):
            PART[i, :, 2 * rows_p + k * rows_d : 2 * rows_p + (k + 1) * rows_d] = wdt[:, k * FC : (k + 1) * FC].reshape(2 * n, rows_d, FC)
        events(i, 1, 1)
        gw = dot(AT[...], DGU[...]).astype(bf16)
        PART[i, :, 0:rows_p] = gw[:, :FC].reshape(2 * n, rows_p, FC)
        PART[i, :, rows_p : 2 * rows_p] = gw[:, FC:].reshape(2 * n, rows_p, FC)

        for h in (0, 1):
            rs_copy(i, 0, h).start()
        if ly:
            ACC[...] += dot_nt(DGU[...], wgu[...])

    SQ[...] = jnp.zeros_like(SQ)
    loop(chunks, functools.partial(backward, 1, A1))

    def by_input(t):
        r = rows(t)
        w, da = H[r, :].astype(f32), ACC[r, :].astype(bf16).astype(f32)
        s = scale_of(w)
        along = jnp.sum(da * w, -1, keepdims=True) * (s * s * s) * (1.0 / d)
        by_h = (DY[r, :].astype(f32) + (da * s - w * along).astype(bf16).astype(f32)).astype(bf16)
        DY[r, :] = by_h
        DYT[:, r] = by_h.T
        AT[:, r] = A0[r, :].T

    loop(4, by_input)
    loop(chunks, lambda i: backward(0, A0, i + chunks))

    groups = units // JOINT

    def ag_copy(g, j, h):
        us = pl.ds(JOINT * g, JOINT)
        src = PART.at[us, 2 * me + h] if isinstance(j, int) and j == 0 else G.at[h, j, us]
        dst = last[h].at[us] if isinstance(j, int) and j == rounds - 1 else G.at[h, j + 1, us]
        return pltpu.make_async_remote_copy(src, dst, ag_s.at[g], ag_r.at[g, j], device_id=(rep, to[h]), device_id_type=MESH)

    def ag_wait(g, j):
        whole(RECV.at[0:JOINT, 0], ag_r.at[g, j]).wait()

    def drain(i):
        def one(q):
            u = units + i - n + 1 + q
            s = n - 1 - q

            @pl.when(u < units)
            def _():
                rs_event(u, s)

        loop(n - 1, one)

        def first(k):
            g = groups * i // (n - 1) + k

            @pl.when(g < groups * (i + 1) // (n - 1))
            def _():
                for h in (0, 1):
                    ag_copy(g, 0, h).start()

        loop(-(-groups // (n - 1)), first)

    loop(n - 1, drain)

    lanes = SQA.shape[-1]
    q = SQ[...]
    q = sum(q[:, k * lanes : (k + 1) * lanes] for k in range(FC // lanes))
    SQA[me] = q.reshape(-1, 8, lanes).sum(0)

    def sq_copy(k):
        return pltpu.make_async_remote_copy(SQA.at[me], SQA.at[me], sq_sem.at[0], sq_sem.at[1], device_id=(rep, lax.rem(me + k, n)), device_id_type=MESH)

    for k in range(1, n):
        sq_copy(k).start()

    def gather(t):
        j, g = t // groups, lax.rem(t, groups)
        ag_wait(g, j)
        for h in (0, 1):
            ag_copy(g, j + 1, h).start()

    loop((rounds - 2) * groups, gather)

    def gather_last(g):
        ag_wait(g, rounds - 2)
        for h in (0, 1):
            ag_copy(g, rounds - 1, h).start()

    loop(groups, gather_last)
    whole(SQA.at[1:n], sq_sem.at[1]).wait()
    total = SQA[0]
    for k in range(1, n):
        total = total + SQA[k]
    SQO[...] = jnp.broadcast_to(jnp.sum(total, keepdims=True), SQO.shape)
    sq_copy_out = pltpu.make_async_copy(SQO, sq_out, own_sem.at[1])

    def finish(u):
        whole(RECV.at[u], rs_s.at[u]).wait()

    def finish_ag(g):
        ag_wait(g, rounds - 1)
        whole(RECV.at[0:JOINT, 0:rounds], ag_s.at[g]).wait()

    loop(units, finish)
    sq_copy_out.start()
    loop(groups, finish_ag)
    sq_copy_out.wait()
    whole(RECV.at[:, 0], own_sem.at[0]).wait()
    whole(SQA.at[1:n], sq_sem.at[0]).wait()


def train(n, rounds, x, dy, w_gate, w_up, w_down):
    _, tokens, d = x.shape
    layers, _, ff = w_gate.shape
    units, rows = layers * ff // FC, 3 * d // (2 * n)
    part = (rows, FC)
    any_ = pl.BlockSpec(memory_space=pl.ANY)
    got = jax.ShapeDtypeStruct((units,) + part, bf16)
    act = pltpu.VMEM((tokens, d), bf16)
    act_t = pltpu.VMEM((d, tokens), bf16)
    dma = pltpu.SemaphoreType.DMA
    return pl.pallas_call(
        functools.partial(train_kernel, n, rounds),
        name="train",
        out_shape=(jax.ShapeDtypeStruct((2, rounds, units) + part, bf16), got, got, jax.ShapeDtypeStruct((8, 128), f32)),
        in_specs=[any_] * 5,
        out_specs=(any_,) * 4,
        scratch_shapes=[
            act, act, act_t, act, act, act_t,
            pltpu.VMEM((tokens, d), f32),
            pltpu.VMEM((tokens, FC), bf16),
            pltpu.VMEM((tokens, 2 * FC), bf16),
            pltpu.VMEM((SLOTS // 2, d, 4 * FC), bf16),
            pltpu.VMEM((SLOTS, FC, d), bf16),
            pltpu.VMEM((units, 2 * n) + part, bf16),
            pltpu.VMEM((units, n - 1, 2) + part, bf16),
            pltpu.VMEM(part, f32),
            pltpu.VMEM((n, 8, 128), f32),
            pltpu.VMEM((8, 128), f32),
            dma((5,)), dma((SLOTS, 3)),
            dma((units,)), dma((units, n - 1)), dma((units // JOINT,)), dma((units // JOINT, rounds)), dma((2,)), dma((2,)),
        ],
        compiler_params=pltpu.CompilerParams(collective_id=0, has_side_effects=True, vmem_limit_bytes=67043328),
        cost_estimate=pl.CostEstimate(flops=17 * 2 * tokens * d * ff, bytes_accessed=8 * units * n * rows * FC, transcendentals=0),
    )(x, dy, w_gate, w_up, w_down)


def place_of(k, me, n, layers, first):
    t = first + k // layers
    h, j = lax.rem(t, 2), t // 2
    return lax.rem(k, layers), 2 * lax.rem(me + (2 * h - 1) * j + n, n) + h


def stage_kernel(n, first, *refs):
    arrays, wide, tall, sem = refs[:9], refs[9:12], refs[12:15], refs[15]
    layers, steps = arrays[0].shape[0], wide[0].shape[0]
    me = lax.axis_index("dp")

    def copies(k):
        ly, p = place_of(k, me, n, layers, first)
        for q in range(3):
            for x in range(3):
                here = tall[q].at[k] if x == 2 else wide[q].at[k, x]
                there = arrays[3 * q + x].at[ly, :, p] if x == 2 else arrays[3 * q + x].at[ly, p]
                yield pltpu.make_async_copy(there, here, sem.at[q, x])

    def start(k):
        for c in copies(k):
            c.start()

    loop(steps, start)
    for q in range(3):
        for x in range(2):
            both = wide[q].at[:, x]
            pltpu.make_async_copy(both, both, sem.at[q, x]).wait()
        pltpu.make_async_copy(tall[q], tall[q], sem.at[q, 2]).wait()


def stage(views, first, steps, n):
    w, m, v = views
    _, _, rows_p, ff = w[0].shape
    _, chunks, _, rows_d, d = w[2].shape
    types = (bf16, f32, f32)
    shapes = [jax.ShapeDtypeStruct((steps, 2, rows_p, ff), t) for t in types] + [jax.ShapeDtypeStruct((steps, chunks, rows_d, d), t) for t in types]
    return pl.pallas_call(
        functools.partial(stage_kernel, n, first),
        name="stage",
        in_specs=[pl.BlockSpec(memory_space=pltpu.HBM)] * 9,
        out_specs=[pl.BlockSpec(memory_space=pltpu.VMEM)] * 6,
        out_shape=shapes,
        scratch_shapes=[pltpu.SemaphoreType.DMA((3, 3))],
        compiler_params=pltpu.CompilerParams(vmem_limit_bytes=40 << 20),
        cost_estimate=pl.CostEstimate(flops=3000000000, bytes_accessed=10000000, transcendentals=0),
    )(*w, *m, *v)


def adam_kernel(n, count, sources, n_src, aliased, staged, sq, *refs):
    gs, w, m, v = refs[:n_src], refs[n_src : n_src + 3], refs[n_src + 3 : n_src + 6], refs[n_src + 6 : n_src + 9]
    if staged:
        old_wide, old_tall = refs[n_src : n_src + 3], refs[n_src + 3 : n_src + 6]
        refs = refs[n_src + 6 + (9 if aliased else 0) :]
        w = refs[:3]
    else:
        refs = refs[n_src + 9 + (9 if aliased else 0) :]
    outs, g_in, wide, tall, in_sem, out_sem = refs[:9], refs[9], refs[10:13], refs[13:16], *refs[16:18]
    layers, _, rows_p, _ = w[0].shape
    _, chunks, _, rows_d, d = w[2].shape
    depth = g_in.shape[0]
    steps = layers * len(sources)
    me = lax.axis_index("dp")
    _, h0, j0 = sources[0]

    def place(k):
        return place_of(k, me, n, layers, 2 * j0 + h0)

    def state(k, arrays, sem, out):
        ly, p = place(k)
        slot = lax.rem(k, depth)
        for q in range(3):
            for x in range(3):
                here = tall[q].at[slot] if x == 2 else wide[q].at[slot, x]
                there = arrays[3 * q + x].at[ly, :, p] if x == 2 else arrays[3 * q + x].at[ly, p]
                yield pltpu.make_async_copy(*((here, there) if out else (there, here)), sem.at[slot])

    def taken(k):
        return state(k, (*w, *m, *v), in_sem, False)

    def given(k):
        return state(k, outs, out_sem, True)

    def arrived(k, sem, times):
        slots = g_in.at[0:times]
        pltpu.make_async_copy(slots, slots, sem.at[lax.rem(k, depth)]).wait()

    def gradient(k, x, t):
        units = pl.ds((layers - 1 - lax.rem(k, layers)) * chunks, chunks)
        at = gs[x].at[units]
        if len(gs[x].shape) == 5:
            i = 2 * sources[t][2] + sources[t][1] + k // layers - t
            at = gs[x].at[lax.rem(i, 2), i // 2, units]
        slot = lax.rem(k, depth)
        return pltpu.make_async_copy(at, g_in.at[slot], in_sem.at[slot])

    spans = [[t for t, src in enumerate(sources) if src[0] == x] for x in range(n_src)]

    def start(k):
        for c in taken(k):
            c.start()
        for x, span in enumerate(spans):

            @pl.when((k >= layers * span[0]) & (k < layers * (span[-1] + 1)))
            def _():
                gradient(k, x, span[0]).start()

    if not staged:
        loop(min(depth - 2, steps), start)
    factor = jnp.minimum(1.0, 0.5 * lax.rsqrt(sq[0:1, 0:1] / count + 1e-30))

    def update(g, arrays, old_arrays, at):
        g = g.astype(f32) * factor
        w, m, v = (a.at[at] for a in arrays)
        old_w, old_m, old_v = (a.at[at] for a in old_arrays)
        new_m = 0.9 * old_m[...] + 0.1 * g
        new_v = 0.95 * old_v[...] + 0.05 * g * g
        old = old_w[...].astype(f32)
        m[...] = new_m
        v[...] = new_v
        w[...] = (old - 0.02 * (new_m * lax.rsqrt(new_v + 1e-8) + 0.1 * old)).astype(bf16)

    def step(k):
        slot = lax.rem(k, depth)
        back = layers - 1 - place(k)[0]
        if not staged:
            arrived(k, in_sem, 6)

        def run(g, first):
            def chunk(c):
                cols = pl.ds(pl.multiple_of(c * FC, FC), FC)
                for x in range(2):
                    update(g[first + c, x * rows_p : (x + 1) * rows_p], wide, old_wide if staged else wide, (slot, x, slice(None), cols))
                for x in range(d // FC):
                    at = 2 * rows_p + x * rows_d
                    update(g[first + c, at : at + rows_d], tall, old_tall if staged else tall, (slot, c, slice(None), slice(x * FC, (x + 1) * FC)))

            lax.fori_loop(0, chunks, lambda c, x: (chunk(c), x)[1], 0, unroll=5 if staged else 1)

        if staged:
            for x, span in enumerate(spans):
                pl.when((k >= layers * span[0]) & (k < layers * (span[-1] + 1)))(functools.partial(run, gs[x], back * chunks))
        else:
            run(g_in.at[slot], 0)
        for c in given(k):
            c.start()

        @pl.when(k >= 2)
        def _():
            arrived(k - 2, out_sem, 5)

        if not staged:

            @pl.when(k + depth - 2 < steps)
            def _():
                start(k + depth - 2)

    loop(steps, step)

    def finish(k):
        arrived(steps - 2 + k, out_sem, 5)

    loop(2, finish)


def adam(views, prev, sq, gs, sources, n, count, staged=None, limit=67043328):
    w, m, v = views
    _, parts, rows_p, ff = w[0].shape
    _, chunks, _, rows_d, d = w[2].shape
    any_, vmem = pl.BlockSpec(memory_space=pl.ANY), pl.BlockSpec(memory_space=pltpu.VMEM)
    args = [*gs, *(staged or (*w, *m, *v))]
    aliases = {}
    if prev is not None:
        aliases = {1 + len(args) + k: k for k in range(9)}
        args += list(prev)
    moved = 2 * len(sources) * sum(a.size * a.dtype.itemsize for a in (*w, *m, *v)) // parts
    types = (bf16, f32, f32)
    return pl.pallas_call(
        functools.partial(adam_kernel, n, count, sources, len(gs), prev is not None, bool(staged)),
        name="adam",
        in_specs=[vmem] + [vmem if staged else any_] * len(gs) + [vmem if staged else any_] * (6 if staged else 9) + [any_] * (0 if prev is None else 9),
        out_specs=[any_] * 9,
        out_shape=[jax.ShapeDtypeStruct(a.shape, a.dtype) for a in (*w, *m, *v)],
        input_output_aliases=aliases,
        scratch_shapes=[pltpu.VMEM((DEPTH, chunks, gs[0].shape[-2], FC), bf16)]
        + [pltpu.VMEM((DEPTH, 2, rows_p, ff), t) for t in types]
        + [pltpu.VMEM((DEPTH, chunks, rows_d, d), t) for t in types]
        + [pltpu.SemaphoreType.DMA((DEPTH,)), pltpu.SemaphoreType.DMA((DEPTH,))],
        compiler_params=pltpu.CompilerParams(vmem_limit_bytes=limit),
        cost_estimate=pl.CostEstimate(flops=30 * moved, bytes_accessed=moved, transcendentals=0),
    )(sq, *args)


def solution(mesh):
    n = mesh.shape["dp"]

    def step(x, dy, *arrays):
        w = arrays[0:3]
        count = 3 * w[0].size
        rounds = HELD
        return whole(n, rounds, count, x, dy, arrays)

    def whole(n, rounds, count, x, dy, arrays):
        w = arrays[0:3]
        layers, d, ff = w[0].shape
        G, *got, sq = train(n, rounds, x, dy, *w)

        def view(a):
            a = list(a)
            for k in range(2):
                a[k] = a[k].reshape(layers, 2 * n, d // (2 * n), ff)
            a[2] = a[2].reshape(layers, ff // FC, 2 * n, FC // (2 * n), d)
            return a

        views = tuple(view(arrays[k : k + 3]) for k in (0, 3, 6))
        right, left = [(k, (k + 1) % n) for k in range(n)], [(k, (k - 1) % n) for k in range(n)]

        out, hops = None, n - 1 - rounds
        came, at = [got], 0
        for k in range(hops + 1):
            if k < hops:
                r = lax.ppermute(came[k][0], "dp", right)
                came.append([r, lax.ppermute(came[k][1], "dp", left)])
            gs, sources = [], []
            for p in range(at, at + (-(-(2 * n - 2 - at) // (hops - k)) if k < hops else 2)):
                j, h = p // 2, p % 2
                g = G if j < rounds else came[j - rounds][h]
                if not any(g is o for o in gs):
                    gs.append(g)
                sources.append((len(gs) - 1, h, j))
            at += len(sources)
            out = adam(views, out, sq, gs, sources, n, count, staged if k == hops else None, LIMITS.get(hops - k, 67043328))
            if k == hops - 1:
                staged = stage(views, at, 2 * layers, n)
        return tuple(o.reshape(a.shape) for o, a in zip(out, arrays, strict=True))

    return jax.shard_map(
        step,
        mesh=mesh,
        in_specs=(P(("rep", "dp"), None, None),) * 2 + (P(None, None, None),) * 9,
        out_specs=(P("rep", None, None),) * 9,
        check_vma=False,
    )
```

```python
import functools

import jax
import jax.numpy as jnp
from jax import lax
from jax.experimental import pallas as pl
from jax.experimental.pallas import tpu as pltpu
from jax.sharding import PartitionSpec as P


f32, bf16 = jnp.float32, jnp.bfloat16
MESH = pl.DeviceIdType.MESH
FC = 256
SLOTS = 4
JOINT = 2
HELD = 3
LIMITS = {1: 61 << 20, 0: 24 << 20}
DEPTH = 6
TILE = 1024


def dot(a, b):
    return jnp.dot(a, b, preferred_element_type=f32)


def dot_nt(a, b):
    return lax.dot_general(a, b, (((1,), (1,)), ((), ())), preferred_element_type=f32)


def sigmoid(x):
    return 0.5 * jnp.tanh(0.5 * x) + 0.5


def loop(n, body):
    lax.fori_loop(0, n, lambda i, c: (body(i), c)[1], 0)


def train_kernel(n, rounds, x, dy, wg_h, wu_h, wd_h, G, L0, L1, sq_out, A0, A1, AT, H, DY, DYT, ACC, HID, DGU, WGU, WD, PART, RECV, SQ, SQA, SQO,
                 in_sem, w_sem, rs_s, rs_r, ag_s, ag_r, own_sem, sq_sem):
    _, tokens, d = x.shape
    layers, _, ff = wg_h.shape
    chunks = ff // FC
    units = layers * chunks
    last = (L0, L1)
    rows_p, rows_d = d // (2 * n), FC // (2 * n)
    me, rep = lax.axis_index("dp"), lax.axis_index("rep")
    to = (lax.rem(me + 1, n), lax.rem(me + n - 1, n))
    sign = (-1, 1)
    step_rows = tokens // 4

    bar = pltpu.get_barrier_semaphore()
    for k in range(1, n):
        pl.semaphore_signal(bar, inc=1, device_id=(rep, lax.rem(me + k, n)), device_id_type=MESH)

    def w_copies(i):
        slot = lax.rem(i, SLOTS)
        ly = jnp.where(i // chunks == 1, layers - 1, 0)
        c = pl.ds(pl.multiple_of(lax.rem(i, chunks) * FC, FC), FC)
        half = lax.rem(slot, 2)
        first = i < chunks
        at = jnp.where(first, half, 2 * half) * FC
        gap = jnp.where(first, 2, 1) * FC
        return (
            pltpu.make_async_copy(wg_h.at[ly, :, c], WGU.at[slot // 2, :, pl.ds(pl.multiple_of(at, FC), FC)], w_sem.at[slot, 0]),
            pltpu.make_async_copy(wu_h.at[ly, :, c], WGU.at[slot // 2, :, pl.ds(pl.multiple_of(at + gap, FC), FC)], w_sem.at[slot, 1]),
            pltpu.make_async_copy(wd_h.at[ly, c, :], WD.at[slot], w_sem.at[slot, 2]),
        )

    def w_start(i):
        for c in w_copies(i):
            c.start()

    def w_wait(i):
        for c in w_copies(i):
            c.wait()

    def rows(t):
        return pl.ds(pl.multiple_of(t * step_rows, step_rows), step_rows)

    def x_in(t):
        return pltpu.make_async_copy(x.at[0, rows(t)], H.at[rows(t)], in_sem.at[t])

    dy_in = pltpu.make_async_copy(dy.at[0], DY, in_sem.at[4])
    loop(4, lambda t: x_in(t).start())
    w_start(0)
    w_start(1)
    dy_in.start()

    def scale_of(w):
        return lax.rsqrt(jnp.mean(w * w, -1, keepdims=True) + 1e-6)

    def norm_x(t):
        x_in(t).wait()
        w = H[rows(t), :].astype(f32)
        A0[rows(t), :] = (w * scale_of(w)).astype(bf16)

    loop(4, norm_x)
    ACC[...] = jnp.zeros_like(ACC)

    def forward(i, turn):
        w_wait(2 * i)
        w_wait(2 * i + 1)
        w_start(2 * i + 2)
        w_start(2 * i + 3)
        pair = lax.rem(i, SLOTS // 2)
        a = A0[...]
        g = dot(a, WGU[pair, :, 0 : 2 * FC])
        u = dot(a, WGU[pair, :, 2 * FC : 4 * FC])
        ACC[...] += dot((g * sigmoid(g) * u).astype(bf16), WD[pl.ds(2 * pair, 2)].reshape(2 * FC, d))
        if turn:
            t = rows(lax.rem(i, 4))
            DYT[:, t] = DY[t, :].T

    forward(0, False)
    dy_in.wait()
    loop(chunks // 2 - 1, lambda i: forward(i + 1, True))
    assert chunks // 2 > 4

    def between(t):
        r = rows(t)
        h = (H[r, :].astype(f32) + ACC[r, :].astype(bf16).astype(f32)).astype(bf16)
        H[r, :] = h
        w = h.astype(f32)
        a = (w * scale_of(w)).astype(bf16)
        A1[r, :] = a
        AT[:, r] = a.T
        ACC[r, :] = jnp.zeros((step_rows, d), f32)

    loop(4, between)
    pl.semaphore_wait(bar, n - 1)

    def piece(s, h):
        return 2 * lax.rem(me + sign[h] * (1 + s) + 2 * n, n) + h

    def rs_copy(u, s, h):
        return pltpu.make_async_remote_copy(PART.at[u, piece(s, h)], RECV.at[lax.rem(u, n), s, h], rs_s.at[u], rs_r.at[lax.rem(u, n), s],
                                            device_id=(rep, to[h]), device_id_type=MESH)

    def whole(ref, sem):
        return pltpu.make_async_copy(ref, ref, sem)

    def rs_take(u, s, h):
        p = piece(s + 1, h)
        total = (PART[u, p].astype(f32) + RECV[lax.rem(u, n), s, h].astype(f32)).astype(bf16)
        PART[u, p] = total
        return total

    def rs_event(u, s):
        whole(RECV.at[0, 0], rs_r.at[lax.rem(u, n), s - 1]).wait()

        @pl.when(s < n - 1)
        def _():
            for h in (0, 1):
                rs_take(u, s - 1, h)
            for h in (0, 1):
                rs_copy(u, s, h).start()

        @pl.when(s == n - 1)
        def _():
            for h in (0, 1):
                g = rs_take(u, n - 2, h).astype(f32)
                SQ[...] += g * g
                own_copy(u, h).start()

    def own_copy(u, h):
        return pltpu.make_async_copy(PART.at[u, 2 * me + h], G.at[h, 0, u], own_sem.at[0])

    def events(i, back, number):
        def one(q):
            s = back - q

            @pl.when(i >= s)
            def _():
                rs_event(i - s, s)

        loop(number, one)

    def backward(ly, A, i):
        w_wait(i + chunks)

        @pl.when(i + 2 < units)
        def _():
            w_start(i + chunks + 2)

        slot = lax.rem(i + chunks, SLOTS)
        wgu = WGU.at[slot // 2, :, pl.ds(pl.multiple_of(lax.rem(slot, 2) * 2 * FC, 2 * FC), 2 * FC)]
        wd = WD.at[slot]

        def tile(t):
            r = pl.ds(pl.multiple_of(t * TILE, TILE), TILE)
            gu = dot(A[r, :], wgu[...])
            g, u = gu[:, :FC], gu[:, FC:]
            by_hid = dot_nt(DY[r, :], wd[...]).astype(bf16).astype(f32)
            sg = sigmoid(g)
            sl = g * sg
            HID[r, :] = (sl * u).astype(bf16)
            DGU[r, FC : 2 * FC] = (by_hid * sl).astype(bf16)
            DGU[r, 0:FC] = (by_hid * u * (sg + sl * (1 - sg))).astype(bf16)
            events(i, jnp.where(t == 0, n - 1, (n - 2) // 2), jnp.where(t == 0, n // 2, (n - 2) // 2 - 1))

        loop(tokens // TILE, tile)
        wdt = dot(DYT[...], HID[...]).astype(bf16).T
        for k in range(d // FC):
            PART[i, :, 2 * rows_p + k * rows_d : 2 * rows_p + (k + 1) * rows_d] = wdt[:, k * FC : (k + 1) * FC].reshape(2 * n, rows_d, FC)
        events(i, 1, 1)
        gw = dot(AT[...], DGU[...]).astype(bf16)
        PART[i, :, 0:rows_p] = gw[:, :FC].reshape(2 * n, rows_p, FC)
        PART[i, :, rows_p : 2 * rows_p] = gw[:, FC:].reshape(2 * n, rows_p, FC)

        for h in (0, 1):
            rs_copy(i, 0, h).start()
        if ly:
            ACC[...] += dot_nt(DGU[...], wgu[...])

    SQ[...] = jnp.zeros_like(SQ)
    loop(chunks, functools.partial(backward, 1, A1))

    def by_input(t):
        r = rows(t)
        w, da = H[r, :].astype(f32), ACC[r, :].astype(bf16).astype(f32)
        s = scale_of(w)
        along = jnp.sum(da * w, -1, keepdims=True) * (s * s * s) * (1.0 / d)
        by_h = (DY[r, :].astype(f32) + (da * s - w * along).astype(bf16).astype(f32)).astype(bf16)
        DY[r, :] = by_h
        DYT[:, r] = by_h.T
        AT[:, r] = A0[r, :].T

    loop(4, by_input)
    loop(chunks, lambda i: backward(0, A0, i + chunks))

    groups = units // JOINT

    def ag_copy(g, j, h):
        us = pl.ds(JOINT * g, JOINT)
        src = PART.at[us, 2 * me + h] if isinstance(j, int) and j == 0 else G.at[h, j, us]
        dst = last[h].at[us] if isinstance(j, int) and j == rounds - 1 else G.at[h, j + 1, us]
        return pltpu.make_async_remote_copy(src, dst, ag_s.at[g], ag_r.at[g, j], device_id=(rep, to[h]), device_id_type=MESH)

    def ag_wait(g, j):
        whole(RECV.at[0:JOINT, 0], ag_r.at[g, j]).wait()

    def drain(i):
        def one(q):
            u = units + i - n + 1 + q
            s = n - 1 - q

            @pl.when(u < units)
            def _():
                rs_event(u, s)

        loop(n - 1, one)

        def first(k):
            g = groups * i // (n - 1) + k

            @pl.when(g < groups * (i + 1) // (n - 1))
            def _():
                for h in (0, 1):
                    ag_copy(g, 0, h).start()

        loop(-(-groups // (n - 1)), first)

    loop(n - 1, drain)

    lanes = SQA.shape[-1]
    q = SQ[...]
    q = sum(q[:, k * lanes : (k + 1) * lanes] for k in range(FC // lanes))
    SQA[me] = q.reshape(-1, 8, lanes).sum(0)

    def sq_copy(k):
        return pltpu.make_async_remote_copy(SQA.at[me], SQA.at[me], sq_sem.at[0], sq_sem.at[1], device_id=(rep, lax.rem(me + k, n)), device_id_type=MESH)

    for k in range(1, n):
        sq_copy(k).start()

    def gather(t):
        j, g = t // groups, lax.rem(t, groups)
        ag_wait(g, j)
        for h in (0, 1):
            ag_copy(g, j + 1, h).start()

    loop((rounds - 2) * groups, gather)

    def gather_last(g):
        ag_wait(g, rounds - 2)
        for h in (0, 1):
            ag_copy(g, rounds - 1, h).start()

    loop(groups, gather_last)
    whole(SQA.at[1:n], sq_sem.at[1]).wait()
    total = SQA[0]
    for k in range(1, n):
        total = total + SQA[k]
    SQO[...] = jnp.broadcast_to(jnp.sum(total, keepdims=True), SQO.shape)
    sq_copy_out = pltpu.make_async_copy(SQO, sq_out, own_sem.at[1])

    def finish(u):
        whole(RECV.at[0], rs_s.at[u]).wait()

    def finish_ag(g):
        ag_wait(g, rounds - 1)
        whole(RECV.at[0:JOINT, 0:rounds], ag_s.at[g]).wait()

    loop(units, finish)
    sq_copy_out.start()
    loop(groups, finish_ag)
    sq_copy_out.wait()
    whole(PART.at[:, 0:2], own_sem.at[0]).wait()
    whole(SQA.at[1:n], sq_sem.at[0]).wait()


def train(n, rounds, x, dy, w_gate, w_up, w_down):
    _, tokens, d = x.shape
    layers, _, ff = w_gate.shape
    units, rows = layers * ff // FC, 3 * d // (2 * n)
    part = (rows, FC)
    any_ = pl.BlockSpec(memory_space=pl.ANY)
    got = jax.ShapeDtypeStruct((units,) + part, bf16)
    act = pltpu.VMEM((tokens, d), bf16)
    act_t = pltpu.VMEM((d, tokens), bf16)
    dma = pltpu.SemaphoreType.DMA
    return pl.pallas_call(
        functools.partial(train_kernel, n, rounds),
        name="train",
        out_shape=(jax.ShapeDtypeStruct((2, rounds, units) + part, bf16), got, got, jax.ShapeDtypeStruct((8, 128), f32)),
        in_specs=[any_] * 5,
        out_specs=(any_,) * 4,
        scratch_shapes=[
            act, act, act_t, act, act, act_t,
            pltpu.VMEM((tokens, d), f32),
            pltpu.VMEM((tokens, FC), bf16),
            pltpu.VMEM((tokens, 2 * FC), bf16),
            pltpu.VMEM((SLOTS // 2, d, 4 * FC), bf16),
            pltpu.VMEM((SLOTS, FC, d), bf16),
            pltpu.VMEM((units, 2 * n) + part, bf16),
            pltpu.VMEM((n, n - 1, 2) + part, bf16),
            pltpu.VMEM(part, f32),
            pltpu.VMEM((n, 8, 128), f32),
            pltpu.VMEM((8, 128), f32),
            dma((5,)), dma((SLOTS, 3)),
            dma((units,)), dma((n, n - 1)), dma((units // JOINT,)), dma((units // JOINT, rounds)), dma((2,)), dma((2,)),
        ],
        compiler_params=pltpu.CompilerParams(collective_id=0, has_side_effects=True, vmem_limit_bytes=67043328),
        cost_estimate=pl.CostEstimate(flops=17 * 2 * tokens * d * ff, bytes_accessed=8 * units * n * rows * FC, transcendentals=0),
    )(x, dy, w_gate, w_up, w_down)


def place_of(k, me, n, layers, first):
    t = first + k // layers
    h, j = lax.rem(t, 2), t // 2
    return lax.rem(k, layers), 2 * lax.rem(me + (2 * h - 1) * j + n, n) + h


def stage_kernel(n, first, *refs):
    arrays, wide, tall, sem = refs[:9], refs[9:12], refs[12:15], refs[15]
    layers, steps = arrays[0].shape[0], wide[0].shape[0]
    me = lax.axis_index("dp")

    def copies(k):
        ly, p = place_of(k, me, n, layers, first)
        for q in range(3):
            for x in range(3):
                here = tall[q].at[k] if x == 2 else wide[q].at[k, x]
                there = arrays[3 * q + x].at[ly, :, p] if x == 2 else arrays[3 * q + x].at[ly, p]
                yield pltpu.make_async_copy(there, here, sem.at[q, x])

    def start(k):
        for c in copies(k):
            c.start()

    loop(steps, start)
    for q in range(3):
        for x in range(2):
            both = wide[q].at[:, x]
            pltpu.make_async_copy(both, both, sem.at[q, x]).wait()
        pltpu.make_async_copy(tall[q], tall[q], sem.at[q, 2]).wait()


def stage(views, first, steps, n):
    w, m, v = views
    _, _, rows_p, ff = w[0].shape
    _, chunks, _, rows_d, d = w[2].shape
    types = (bf16, f32, f32)
    shapes = [jax.ShapeDtypeStruct((steps, 2, rows_p, ff), t) for t in types] + [jax.ShapeDtypeStruct((steps, chunks, rows_d, d), t) for t in types]
    return pl.pallas_call(
        functools.partial(stage_kernel, n, first),
        name="stage",
        in_specs=[pl.BlockSpec(memory_space=pltpu.HBM)] * 9,
        out_specs=[pl.BlockSpec(memory_space=pltpu.VMEM)] * 6,
        out_shape=shapes,
        scratch_shapes=[pltpu.SemaphoreType.DMA((3, 3))],
        compiler_params=pltpu.CompilerParams(vmem_limit_bytes=40 << 20),
        cost_estimate=pl.CostEstimate(flops=3000000000, bytes_accessed=10000000, transcendentals=0),
    )(*w, *m, *v)


def adam_kernel(n, count, sources, n_src, aliased, staged, sq, *refs):
    gs, w, m, v = refs[:n_src], refs[n_src : n_src + 3], refs[n_src + 3 : n_src + 6], refs[n_src + 6 : n_src + 9]
    if staged:
        old_wide, old_tall = refs[n_src : n_src + 3], refs[n_src + 3 : n_src + 6]
        refs = refs[n_src + 6 + (9 if aliased else 0) :]
        w = refs[:3]
    else:
        refs = refs[n_src + 9 + (9 if aliased else 0) :]
    outs, g_in, wide, tall, in_sem, out_sem = refs[:9], refs[9], refs[10:13], refs[13:16], *refs[16:18]
    layers, _, rows_p, _ = w[0].shape
    _, chunks, _, rows_d, d = w[2].shape
    depth = g_in.shape[0]
    steps = layers * len(sources)
    me = lax.axis_index("dp")
    _, h0, j0 = sources[0]

    def place(k):
        return place_of(k, me, n, layers, 2 * j0 + h0)

    def state(k, arrays, sem, out):
        ly, p = place(k)
        slot = lax.rem(k, depth)
        for q in range(3):
            for x in range(3):
                here = tall[q].at[slot] if x == 2 else wide[q].at[slot, x]
                there = arrays[3 * q + x].at[ly, :, p] if x == 2 else arrays[3 * q + x].at[ly, p]
                yield pltpu.make_async_copy(*((here, there) if out else (there, here)), sem.at[slot])

    def taken(k):
        return state(k, (*w, *m, *v), in_sem, False)

    def given(k):
        return state(k, outs, out_sem, True)

    def arrived(k, sem, times):
        slots = g_in.at[0:times]
        pltpu.make_async_copy(slots, slots, sem.at[lax.rem(k, depth)]).wait()

    def gradient(k, x, t):
        units = pl.ds((layers - 1 - lax.rem(k, layers)) * chunks, chunks)
        at = gs[x].at[units]
        if len(gs[x].shape) == 5:
            i = 2 * sources[t][2] + sources[t][1] + k // layers - t
            at = gs[x].at[lax.rem(i, 2), i // 2, units]
        slot = lax.rem(k, depth)
        return pltpu.make_async_copy(at, g_in.at[slot], in_sem.at[slot])

    spans = [[t for t, src in enumerate(sources) if src[0] == x] for x in range(n_src)]

    def start(k):
        for c in taken(k):
            c.start()
        for x, span in enumerate(spans):

            @pl.when((k >= layers * span[0]) & (k < layers * (span[-1] + 1)))
            def _():
                gradient(k, x, span[0]).start()

    if not staged:
        loop(min(depth - 2, steps), start)
    factor = jnp.minimum(1.0, 0.5 * lax.rsqrt(sq[0:1, 0:1] / count + 1e-30))

    def update(g, arrays, old_arrays, at):
        g = g.astype(f32) * factor
        w, m, v = (a.at[at] for a in arrays)
        old_w, old_m, old_v = (a.at[at] for a in old_arrays)
        new_m = 0.9 * old_m[...] + 0.1 * g
        new_v = 0.95 * old_v[...] + 0.05 * g * g
        old = old_w[...].astype(f32)
        m[...] = new_m
        v[...] = new_v
        w[...] = (old - 0.02 * (new_m * lax.rsqrt(new_v + 1e-8) + 0.1 * old)).astype(bf16)

    def step(k):
        slot = lax.rem(k, depth)
        back = layers - 1 - place(k)[0]
        if not staged:
            arrived(k, in_sem, 6)

        def run(g, first):
            def chunk(c):
                cols = pl.ds(pl.multiple_of(c * FC, FC), FC)
                for x in range(2):
                    update(g[first + c, x * rows_p : (x + 1) * rows_p], wide, old_wide if staged else wide, (slot, x, slice(None), cols))
                for x in range(d // FC):
                    at = 2 * rows_p + x * rows_d
                    update(g[first + c, at : at + rows_d], tall, old_tall if staged else tall, (slot, c, slice(None), slice(x * FC, (x + 1) * FC)))

            lax.fori_loop(0, chunks, lambda c, x: (chunk(c), x)[1], 0, unroll=5 if staged else 1)

        if staged:
            for x, span in enumerate(spans):
                pl.when((k >= layers * span[0]) & (k < layers * (span[-1] + 1)))(functools.partial(run, gs[x], back * chunks))
        else:
            run(g_in.at[slot], 0)
        for c in given(k):
            c.start()

        @pl.when(k >= 2)
        def _():
            arrived(k - 2, out_sem, 5)

        if not staged:

            @pl.when(k + depth - 2 < steps)
            def _():
                start(k + depth - 2)

    loop(steps, step)

    def finish(k):
        arrived(steps - 2 + k, out_sem, 5)

    loop(2, finish)


def adam(views, prev, sq, gs, sources, n, count, staged=None, limit=67043328):
    w, m, v = views
    _, parts, rows_p, ff = w[0].shape
    _, chunks, _, rows_d, d = w[2].shape
    any_, vmem = pl.BlockSpec(memory_space=pl.ANY), pl.BlockSpec(memory_space=pltpu.VMEM)
    args = [*gs, *(staged or (*w, *m, *v))]
    aliases = {}
    if prev is not None:
        aliases = {1 + len(args) + k: k for k in range(9)}
        args += list(prev)
    moved = 2 * len(sources) * sum(a.size * a.dtype.itemsize for a in (*w, *m, *v)) // parts
    types = (bf16, f32, f32)
    return pl.pallas_call(
        functools.partial(adam_kernel, n, count, sources, len(gs), prev is not None, bool(staged)),
        name="adam",
        in_specs=[vmem] + [vmem if staged else any_] * len(gs) + [vmem if staged else any_] * (6 if staged else 9) + [any_] * (0 if prev is None else 9),
        out_specs=[any_] * 9,
        out_shape=[jax.ShapeDtypeStruct(a.shape, a.dtype) for a in (*w, *m, *v)],
        input_output_aliases=aliases,
        scratch_shapes=[pltpu.VMEM((DEPTH, chunks, gs[0].shape[-2], FC), bf16)]
        + [pltpu.VMEM((DEPTH, 2, rows_p, ff), t) for t in types]
        + [pltpu.VMEM((DEPTH, chunks, rows_d, d), t) for t in types]
        + [pltpu.SemaphoreType.DMA((DEPTH,)), pltpu.SemaphoreType.DMA((DEPTH,))],
        compiler_params=pltpu.CompilerParams(vmem_limit_bytes=limit),
        cost_estimate=pl.CostEstimate(flops=30 * moved, bytes_accessed=moved, transcendentals=0),
    )(sq, *args)


def solution(mesh):
    n = mesh.shape["dp"]

    def step(x, dy, *arrays):
        w = arrays[0:3]
        count = 3 * w[0].size
        rounds = HELD
        return whole(n, rounds, count, x, dy, arrays)

    def whole(n, rounds, count, x, dy, arrays):
        w = arrays[0:3]
        layers, d, ff = w[0].shape
        G, *got, sq = train(n, rounds, x, dy, *w)

        def view(a):
            a = list(a)
            for k in range(2):
                a[k] = a[k].reshape(layers, 2 * n, d // (2 * n), ff)
            a[2] = a[2].reshape(layers, ff // FC, 2 * n, FC // (2 * n), d)
            return a

        views = tuple(view(arrays[k : k + 3]) for k in (0, 3, 6))
        right, left = [(k, (k + 1) % n) for k in range(n)], [(k, (k - 1) % n) for k in range(n)]

        out, hops = None, n - 1 - rounds
        came, at = [got], 0
        for k in range(hops + 1):
            if k < hops:
                r = lax.ppermute(came[k][0], "dp", right)
                came.append([r, lax.ppermute(came[k][1], "dp", left)])
            gs, sources = [], []
            for p in range(at, at + (-(-(2 * n - 2 - at) // (hops - k)) if k < hops else 2)):
                j, h = p // 2, p % 2
                g = G if j < rounds else came[j - rounds][h]
                if not any(g is o for o in gs):
                    gs.append(g)
                sources.append((len(gs) - 1, h, j))
            at += len(sources)
            out = adam(views, out, sq, gs, sources, n, count, staged if k == hops else None, LIMITS.get(hops - k, 67043328))
            if k == hops - 1:
                staged = stage(views, at, 2 * layers, n)
        return tuple(o.reshape(a.shape) for o, a in zip(out, arrays, strict=True))

    return jax.shard_map(
        step,
        mesh=mesh,
        in_specs=(P(("rep", "dp"), None, None),) * 2 + (P(None, None, None),) * 9,
        out_specs=(P("rep", None, None),) * 9,
        check_vma=False,
    )
```
